32 devices in a mesh: dp: 1 (over z), sp: 32 (over y, x, core).
Axes of the slice: x: 4, y: 4, z: 1, core: 2. Of those that a mesh axis runs over, the one named last changes fastest.
The devices are a block of a 4x4x8 slice.
Arguments:
- patches: bfloat16 [16, 16384, 768], P('dp', 'sp')
- ln1_scale: float32 [768], replicated
- ln1_bias: float32 [768], replicated
- w_tok1: bfloat16 [16384, 384], replicated
- b_tok1: float32 [384], replicated
- w_tok2: bfloat16 [384, 16384], replicated
- b_tok2: float32 [16384], replicated
- ln2_scale: float32 [768], replicated
- ln2_bias: float32 [768], replicated
- w_ch1: bfloat16 [768, 3072], replicated
- b_ch1: float32 [3072], replicated
- w_ch2: bfloat16 [3072, 768], replicated
- b_ch2: float32 [768], replicated
Outputs:
- output: bfloat16 [16, 16384, 768], P('dp', 'sp')
All inputs are finite; a program needn't handle non-finite values.
Results may differ from the reference program's by a relative error of at most 0.0112.
Values are sent between devices in bfloat16 or wider.
A program may use at most 768 MiB of HBM per device.

```python
import jax
import jax.numpy as jnp
from jax import lax

BATCH = 16
SEQ_DEV = 512
GROUP = 32
CHANNELS = 768
TOK_HIDDEN = 384
CH_HIDDEN = 3072
SEQ_LEN = SEQ_DEV * GROUP
LN_EPS = 1e-6


def layer_norm(rows, scale, offset):
    rows_wide = rows.astype(jnp.float32)
    row_mean = jnp.mean(rows_wide, axis=-1, keepdims=True)
    centered = rows_wide - row_mean
    row_var = jnp.mean(centered * centered, axis=-1, keepdims=True)
    return (centered * lax.rsqrt(row_var + LN_EPS) * scale + offset).astype(jnp.bfloat16)


def setup_inputs(seed: int = 0, part: int = 0) -> dict:
    keys = jax.random.split(jax.random.key(seed), 13)

    def draw_normal(index, shape):
        return jax.random.normal(keys[index], shape, jnp.float32)

    patches = jax.random.normal(jax.random.fold_in(keys[0], part), (BATCH, SEQ_LEN, CHANNELS), jnp.float32)
    return dict(
        patches=patches.astype(jnp.bfloat16),
        ln1_scale=1.0 + 0.3 * draw_normal(1, (CHANNELS,)),
        ln1_bias=0.3 * draw_normal(2, (CHANNELS,)),
        w_tok1=(draw_normal(3, (SEQ_LEN, TOK_HIDDEN)) * SEQ_LEN ** -0.5).astype(jnp.bfloat16),
        b_tok1=0.5 * draw_normal(4, (TOK_HIDDEN,)),
        w_tok2=(draw_normal(5, (TOK_HIDDEN, SEQ_LEN)) * TOK_HIDDEN ** -0.5).astype(jnp.bfloat16),
        b_tok2=0.5 * draw_normal(6, (SEQ_LEN,)),
        ln2_scale=1.0 + 0.3 * draw_normal(7, (CHANNELS,)),
        ln2_bias=0.3 * draw_normal(8, (CHANNELS,)),
        w_ch1=(draw_normal(9, (CHANNELS, CH_HIDDEN)) * CHANNELS ** -0.5).astype(jnp.bfloat16),
        b_ch1=0.5 * draw_normal(10, (CH_HIDDEN,)),
        w_ch2=(draw_normal(11, (CH_HIDDEN, CHANNELS)) * CH_HIDDEN ** -0.5).astype(jnp.bfloat16),
        b_ch2=0.5 * draw_normal(12, (CHANNELS,)),
    )


def reference(patches, ln1_scale, ln1_bias, w_tok1, b_tok1, w_tok2, b_tok2, ln2_scale, ln2_bias, w_ch1, b_ch1, w_ch2, b_ch2):
    w_tok2_blocks = jnp.transpose(w_tok2.reshape(TOK_HIDDEN, GROUP, SEQ_DEV), (1, 0, 2))
    b_tok2_blocks = b_tok2.reshape(GROUP, SEQ_DEV)

    def one_image(image):
        normed = layer_norm(image, ln1_scale, ln1_bias)
        hidden = jnp.dot(w_tok1.T, normed, preferred_element_type=jnp.float32) + b_tok1[:, None]
        act_tok = jax.nn.gelu(hidden, approximate=True).astype(jnp.bfloat16)
        image_blocks = image.reshape(GROUP, SEQ_DEV, CHANNELS)

        def one_block(block_args):
            rows, w_rows, b_rows = block_args
            mixed = (jnp.dot(w_rows.T, act_tok, preferred_element_type=jnp.float32) + b_rows[:, None]).astype(jnp.bfloat16)
            residual = (rows.astype(jnp.float32) + mixed.astype(jnp.float32)).astype(jnp.bfloat16)
            chan_in = layer_norm(residual, ln2_scale, ln2_bias)
            pre_act = jnp.dot(chan_in, w_ch1, preferred_element_type=jnp.float32) + b_ch1
            act_ch = jax.nn.gelu(pre_act, approximate=True).astype(jnp.bfloat16)
            ch_out = jnp.dot(act_ch, w_ch2, preferred_element_type=jnp.float32) + b_ch2
            return (residual.astype(jnp.float32) + ch_out).astype(jnp.bfloat16)

        out_blocks = lax.map(one_block, (image_blocks, w_tok2_blocks, b_tok2_blocks))
        return out_blocks.reshape(SEQ_LEN, CHANNELS)

    return lax.map(one_image, patches)
```

```python
import functools
import math

import jax
import jax.numpy as jnp
from jax import lax
from jax.experimental import pallas as pl
from jax.experimental.pallas import tpu as pltpu
from jax.sharding import PartitionSpec as P

LN_EPS = 1e-6
K0 = math.sqrt(2.0 / math.pi)
K1 = K0 * 0.044715
MESH = pl.DeviceIdType.MESH
ANY = pl.BlockSpec(memory_space=pl.ANY)
VMEM = pl.BlockSpec(memory_space=pltpu.VMEM)
USLOTS = 4


def layer_norm(rows_wide, scale, offset):
    mean = jnp.mean(rows_wide, axis=-1, keepdims=True)
    centered = rows_wide - mean
    var = jnp.mean(centered * centered, axis=-1, keepdims=True)
    return (centered * lax.rsqrt(var + LN_EPS) * scale + offset).astype(jnp.bfloat16)


def gelu(a):
    half = a * 0.5
    return half * jnp.tanh(a * ((a * a) * K1 + K0)) + half


def dot(a, b):
    return jnp.dot(a, b, preferred_element_type=jnp.float32)


def rows(start, size, align):
    return pl.ds(pl.multiple_of(start, align), size)


def exchange_kernel(side, x_hbm, s1_ref, o1_ref, wt1_hbm, bt1_ref, wt2_hbm, bt2_hbm,
                    g_out, wt2t_ref, bt2c_ref,
                    xbuf, usend, ubuf, hbuf, ra1, ra2, rb1, rb2, gbuf, wt1, wt1t, wt2, bt2, b1c,
                    ssem, rsem, xsem, wsem, osem, credit):
    B, S, C = x_hbm.shape
    pairs = B // 2
    D = wt1_hbm.shape[1]
    DA, DB, CB = D // side, D // side // 2, C // 2

    me = lax.axis_index("sp")
    core = me % 2
    chip = me // 2
    cx, cy = chip % side, chip // side
    a = cx * (1 - core) + cy * core
    b = cy * (1 - core) + cx * core

    def index(ia, ib):
        ix = ia * (1 - core) + ib * core
        iy = ib * (1 - core) + ia * core
        return (iy * side + ix) * 2 + core

    ar, al, ao = (a + 1) % side, (a + side - 1) % side, (a + 2) % side
    br, bl, bo = (b + 1) % side, (b + side - 1) % side, (b + 2) % side
    dev_ar, dev_al = index(ar, b), index(al, b)
    dev_br, dev_bl = index(a, br), index(a, bl)
    partner = me + 1 - 2 * core

    def remote(k, p, src, dst, dev):
        return pltpu.make_async_remote_copy(
            src_ref=src, dst_ref=dst, send_sem=ssem.at[k, p], recv_sem=rsem.at[k, p],
            device_id={"sp": dev}, device_id_type=MESH)

    def sub(j, off=0, size=None):
        return (rows(a * DA + (j // 2) * DB + off, size or DB, 8), rows((j % 2) * CB, CB, 128))

    mine = core

    def d_u(p):
        return remote(0, p, usend.at[p % 2], ubuf.at[p % USLOTS, rows(core * S, S, 16)], partner)

    def d_a1(p):
        return (remote(1, p, hbuf.at[p, rows(ao * DA, DB, 8)], ra1.at[p, 0], dev_ar),
                remote(2, p, hbuf.at[p, rows(ao * DA + DB, DB, 8)], ra1.at[p, 1], dev_al))

    def d_a2(p):
        return (remote(3, p, hbuf.at[p, rows(ar * DA, DA, 8)], ra2.at[p, 0], dev_ar),
                remote(4, p, hbuf.at[p, rows(al * DA, DA, 8)], ra2.at[p, 1], dev_al))

    def d_b1(p):
        return (remote(5, p, hbuf.at[(p, *sub(bo, 0, DB // 2))], rb1.at[p, 0], dev_br),
                remote(6, p, hbuf.at[(p, *sub(bo, DB // 2, DB // 2))], rb1.at[p, 1], dev_bl))

    def d_b2(p):
        return (remote(7, p, hbuf.at[(p, *sub(br))], rb2.at[p, 0], dev_br),
                remote(8, p, hbuf.at[(p, *sub(bl))], rb2.at[p, 1], dev_bl))

    def d_g1(p):
        here = gbuf.at[(p, mine, *sub(b))]
        return remote(9, p, here, here, dev_br), remote(10, p, here, here, dev_bl)

    def d_g2(p):
        top = gbuf.at[(p, mine, *sub(bl, 0, 32))]
        bottom = gbuf.at[(p, mine, *sub(br, 32, DB - 32))]
        return remote(11, p, top, top, dev_br), remote(12, p, bottom, bottom, dev_bl)

    def d_g3(p):
        here = gbuf.at[p, mine, rows(a * DA, DA, 16)]
        return remote(13, p, here, here, dev_ar), remote(14, p, here, here, dev_al)

    def d_g4(p):
        top = gbuf.at[p, mine, rows(al * DA, DB, 16)]
        bottom = gbuf.at[p, mine, rows(ar * DA + DB, DB, 16)]
        return remote(15, p, top, top, dev_ar), remote(16, p, bottom, bottom, dev_al)

    def d_g5(p):
        here = gbuf.at[p, mine]
        return remote(17, p, here, here, partner)

    def d_x(p):
        return (pltpu.make_async_copy(x_hbm.at[2 * p + 1 - core], xbuf.at[p % 2, 0], xsem.at[p % 2, 0]),
                pltpu.make_async_copy(x_hbm.at[2 * p + core], xbuf.at[p % 2, 1], xsem.at[p % 2, 1]))

    def d_out(p):
        return pltpu.make_async_copy(gbuf.at[p], g_out.at[p], osem.at[p])

    w_copies = (pltpu.make_async_copy(wt1_hbm.at[rows(chip * 2 * S, 2 * S, 16)], wt1, wsem.at[0]),
                pltpu.make_async_copy(wt2_hbm.at[:, rows(me * S, S, 128)], wt2, wsem.at[1]),
                pltpu.make_async_copy(bt2_hbm.at[:, rows(me * S, S, 128)], bt2, wsem.at[2]))

    def start(ds):
        for d in ds:
            d.start()

    def wait_recv(ds):
        for d in ds:
            d.wait_recv()

    LT = min(S, 64)

    def ln1(p):
        @pl.when(p + 1 < pairs)
        def _():
            start(d_x(p + 1))

        other, own = d_x(p)
        other.wait()

        @pl.when(p >= 2)
        def _():
            d_u(p - 2).wait_send()

        @pl.loop(0, S // LT)
        def _(i):
            r = rows(i * LT, LT, LT)
            usend[p % 2, r, :] = layer_norm(xbuf[p % 2, 0, r, :].astype(jnp.float32), s1_ref[...], o1_ref[...])

        @pl.when(p >= USLOTS)
        def _():
            pl.semaphore_wait(credit, 1)

        d_u(p).start()
        own.wait()

        @pl.loop(0, S // LT)
        def _(i):
            r = rows(i * LT, LT, LT)
            ubuf[p % USLOTS, rows(core * S + i * LT, LT, LT), :] = layer_norm(
                xbuf[p % 2, 1, r, :].astype(jnp.float32), s1_ref[...], o1_ref[...])

    def mm1(p):
        d_u(p).wait_recv()
        hbuf[p] = dot(wt1t[...], ubuf[p % USLOTS])

        @pl.when(p + USLOTS < pairs)
        def _():
            pl.semaphore_signal(credit, inc=1, device_id={"sp": partner}, device_id_type=MESH)

        start(d_a1(p))

    def a2(p):
        wait_recv(d_a1(p))
        hbuf[p, rows(ar * DA, DB, 8), :] += ra1[p, 0]
        hbuf[p, rows(al * DA + DB, DB, 8), :] += ra1[p, 1]
        start(d_a2(p))

    def b1(p):
        wait_recv(d_a2(p))
        hbuf[p, rows(a * DA, DA, 8), :] += ra2[p, 0] + ra2[p, 1]
        start(d_b1(p))

    def b2(p):
        wait_recv(d_b1(p))
        hbuf[(p, *sub(br, 0, DB // 2))] += rb1[p, 0]
        hbuf[(p, *sub(bl, DB // 2, DB // 2))] += rb1[p, 1]
        start(d_b2(p))

    def g1(p):
        wait_recv(d_b2(p))
        h = hbuf[(p, *sub(b))] + (rb2[p, 0] + rb2[p, 1])
        bias = b1c[rows(a * DA + (b // 2) * DB, DB, 8), 0:1]
        r, c = sub(b)
        gbuf[p, mine, rows(a * DA + (b // 2) * DB, DB, 16), c] = gelu(h + bias).astype(jnp.bfloat16)
        start(d_g1(p))

    def g2(p):
        wait_recv(d_g1(p))
        start(d_g2(p))

    def g3(p):
        wait_recv(d_g2(p))
        start(d_g3(p))

    def g4(p):
        wait_recv(d_g3(p))
        start(d_g4(p))

    def g5(p):
        wait_recv(d_g4(p))
        d_g5(p).start()

    def g6(p):
        d_g5(p).wait_recv()
        d_out(p).start()

    stages = (ln1, mm1, a2, b1, b2, g1, g2, g3, g4, g5, g6)

    start(w_copies)
    start(d_x(0))
    barrier = pltpu.get_barrier_semaphore()
    neighbours = (dev_ar, dev_al, dev_br, dev_bl, partner)
    for dev in neighbours:
        pl.semaphore_signal(barrier, inc=1, device_id={"sp": dev}, device_id_type=MESH)
    b1c[...] = jnp.transpose(jnp.broadcast_to(bt1_ref[...], (128, D)))
    for w in w_copies:
        w.wait()
    wt1t[...] = jnp.transpose(wt1[...])
    wt2t_ref[...] = jnp.transpose(wt2[...])
    bt2c_ref[...] = jnp.transpose(jnp.broadcast_to(bt2[...], (128, S)))
    pl.semaphore_wait(barrier, len(neighbours))

    @pl.loop(0, pairs + len(stages) - 1)
    def _(t):
        for s in reversed(range(len(stages))):
            @pl.when((t >= s) & (t - s < pairs))
            def _():
                stages[s](t - s)

    for p in (pairs - 2, pairs - 1):
        d_u(p).wait_send()

    @pl.loop(0, pairs)
    def _(p):
        for make in (d_a1, d_a2, d_b1, d_b2, d_g1, d_g2, d_g3, d_g4):
            for d in make(p):
                d.wait_send()
        d_g5(p).wait_send()
        d_out(p).wait()


def exchange(side, patches, s1, o1, w_tok1, b_tok1, w_tok2, b_tok2):
    B, S, C = patches.shape
    pairs = B // 2
    D = w_tok1.shape[1]
    DA, DB, CB = D // side, D // side // 2, C // 2
    f32, bf16 = jnp.float32, jnp.bfloat16
    return pl.pallas_call(
        functools.partial(exchange_kernel, side),
        out_shape=(jax.ShapeDtypeStruct((pairs, 2, D, C), bf16),
                   jax.ShapeDtypeStruct((S, D), bf16),
                   jax.ShapeDtypeStruct((S, 128), f32)),
        in_specs=[ANY, VMEM, VMEM, ANY, VMEM, ANY, ANY],
        out_specs=(ANY, VMEM, VMEM),
        scratch_shapes=[
            pltpu.VMEM((2, 2, S, C), bf16),
            pltpu.VMEM((2, S, C), bf16),
            pltpu.VMEM((USLOTS, 2 * S, C), bf16),
            pltpu.VMEM((pairs, D, C), f32),
            pltpu.VMEM((pairs, 2, DB, C), f32),
            pltpu.VMEM((pairs, 2, DA, C), f32),
            pltpu.VMEM((pairs, 2, DB // 2, CB), f32),
            pltpu.VMEM((pairs, 2, DB, CB), f32),
            pltpu.VMEM((pairs, 2, D, C), bf16),
            pltpu.VMEM((2 * S, D), bf16),
            pltpu.VMEM((D, 2 * S), bf16),
            pltpu.VMEM((D, S), bf16),
            pltpu.VMEM((1, S), f32),
            pltpu.VMEM((D, 128), f32),
            pltpu.SemaphoreType.DMA((18, pairs)),
            pltpu.SemaphoreType.DMA((18, pairs)),
            pltpu.SemaphoreType.DMA((2, 2)),
            pltpu.SemaphoreType.DMA((3,)),
            pltpu.SemaphoreType.DMA((pairs,)),
            pltpu.SemaphoreType.REGULAR,
        ],
        compiler_params=pltpu.CompilerParams(collective_id=0, has_side_effects=True, vmem_limit_bytes=60 << 20),
        name="exchange",
    )(patches, s1, o1, w_tok1, b_tok1, w_tok2, b_tok2)


def mixer_kernel(hc, x_ref, g_ref, wt2_ref, bt2_ref, s2_ref, o2_ref, w1_ref, c1_ref, w2_ref, c2_ref, out_ref,
                 v_scr, q_scr, x1_scr, acc):
    H = w1_ref.shape[1]
    t = (dot(wt2_ref[...], g_ref[0]) + bt2_ref[:, 0:1]).astype(jnp.bfloat16)
    x1 = (x_ref[0].astype(jnp.float32) + t.astype(jnp.float32)).astype(jnp.bfloat16)
    x1_scr[...] = x1
    v_scr[...] = layer_norm(x1.astype(jnp.float32), s2_ref[...], o2_ref[...])
    steps = H // hc
    for c in range(steps + 1):
        if c < steps:
            h = pl.ds(c * hc, hc)
            q_scr[:, h] = gelu(dot(v_scr[...], w1_ref[:, h]) + c1_ref[:, h]).astype(jnp.bfloat16)
        if c >= 1:
            h = pl.ds((c - 1) * hc, hc)
            part = dot(q_scr[:, h], w2_ref[h, :])
            if c == 1:
                acc[...] = part + c2_ref[...]
            elif c < steps:
                acc[...] += part
            else:
                out_ref[0] = (x1_scr[...].astype(jnp.float32) + (acc[...] + part)).astype(jnp.bfloat16)


def mixer(patches, g, wt2t, bt2c, s2, o2, w_ch1, b_ch1, w_ch2, b_ch2):
    B, S, C = patches.shape
    D = g.shape[1]
    H = w_ch1.shape[1]

    def const(*shape):
        return pl.BlockSpec(shape, lambda i: (0,) * len(shape), pipeline_mode=pl.Buffered(1))

    return pl.pallas_call(
        functools.partial(mixer_kernel, min(512, H // 2)),
        grid=(B,),
        in_specs=[pl.BlockSpec((1, S, C), lambda i: (i, 0, 0)), pl.BlockSpec((1, D, C), lambda i: (i, 0, 0)),
                  const(S, D), const(S, 128), const(1, C), const(1, C), const(C, H), const(1, H), const(H, C), const(1, C)],
        out_specs=pl.BlockSpec((1, S, C), lambda i: (i, 0, 0)),
        out_shape=jax.ShapeDtypeStruct((B, S, C), jnp.bfloat16),
        scratch_shapes=[pltpu.VMEM((S, C), jnp.bfloat16), pltpu.VMEM((S, H), jnp.bfloat16),
                        pltpu.VMEM((S, C), jnp.bfloat16), pltpu.VMEM((S, C), jnp.float32)],
        compiler_params=pltpu.CompilerParams(vmem_limit_bytes=60 << 20),
        name="mixer",
    )(patches, g, wt2t, bt2c, s2, o2, w_ch1, b_ch1, w_ch2, b_ch2)


def solution(mesh):
    row_spec = P('dp', 'sp', None)
    side = math.isqrt(mesh.shape['sp'] // 2)

    def local_layer(patches, ln1_scale, ln1_bias, w_tok1, b_tok1, w_tok2, b_tok2, ln2_scale, ln2_bias, w_ch1, b_ch1, w_ch2, b_ch2):
        B, S, C = patches.shape
        g, wt2t, bt2c = exchange(side, patches, ln1_scale[None], ln1_bias[None], w_tok1, b_tok1[None], w_tok2, b_tok2[None])
        return mixer(patches, g.reshape(B, -1, C), wt2t, bt2c, ln2_scale[None], ln2_bias[None],
                     w_ch1, b_ch1[None], w_ch2, b_ch2[None])

    return jax.shard_map(local_layer, mesh=mesh, in_specs=(row_spec,) + (P(),) * 12, out_specs=row_spec, check_vma=False)
```

```python
import functools
import math

import jax
import jax.numpy as jnp
from jax import lax
from jax.experimental import pallas as pl
from jax.experimental.pallas import tpu as pltpu
from jax.sharding import PartitionSpec as P

LN_EPS = 1e-6
K0 = math.sqrt(2.0 / math.pi)
K1 = K0 * 0.044715
MESH = pl.DeviceIdType.MESH
ANY = pl.BlockSpec(memory_space=pl.ANY)
VMEM = pl.BlockSpec(memory_space=pltpu.VMEM)
USLOTS = 4
FIRST, PERIOD = 9, 4
A1, A2, B1, B2 = (1, -1), (2, 0), (3, 2), (4, 3)
G1, G2, G3, G4, G5, G6 = (5, 4), (6, 5), (7, 6), (8, 7), (9, 8), (11, 9)


def layer_norm(rows_wide, scale, offset):
    mean = jnp.mean(rows_wide, axis=-1, keepdims=True)
    centered = rows_wide - mean
    var = jnp.mean(centered * centered, axis=-1, keepdims=True)
    return (centered * lax.rsqrt(var + LN_EPS) * scale + offset).astype(jnp.bfloat16)


def gelu(a):
    half = a * 0.5
    return half * jnp.tanh(a * ((a * a) * K1 + K0)) + half


def dot(a, b):
    return jnp.dot(a, b, preferred_element_type=jnp.float32)


def row(ref, cols=slice(None)):
    return ref[cols][None, :]


def rows(start, size, align):
    return pl.ds(pl.multiple_of(start, align), size)


def exchange_kernel(side, done_pairs, x_hbm, s1_ref, o1_ref, wt1_hbm, bt1_ref, wt2_hbm, bt2_hbm,
                    s2_ref, o2_ref, w1_hbm, c1_ref, w2_hbm, c2_ref,
                    out_hbm, g_out, wt2t_ref, bt2c_ref,
                    xbuf, usend, ubuf, hbuf, ra1, ra2, rb1, rb2, gbuf, wt1t, wt2, bt2, b1c,
                    w1, w2, xres, obuf, v_scr, q_scr, x1_scr, acc,
                    ssem, rsem, xsem, wsem, osem, xrsem, obsem, credit):
    B, S, C = x_hbm.shape
    pairs = B // 2
    D = wt1_hbm.shape[1]
    DA, DB, CB = D // side, D // side // 2, C // 2

    me = lax.axis_index("sp")
    core = me % 2
    chip = me // 2
    cx, cy = chip % side, chip // side
    a = cx * (1 - core) + cy * core
    b = cy * (1 - core) + cx * core

    def index(ia, ib):
        ix = ia * (1 - core) + ib * core
        iy = ib * (1 - core) + ia * core
        return (iy * side + ix) * 2 + core

    ar, al, ao = (a + 1) % side, (a + side - 1) % side, (a + 2) % side
    br, bl, bo = (b + 1) % side, (b + side - 1) % side, (b + 2) % side
    dev_ar, dev_al = index(ar, b), index(al, b)
    dev_br, dev_bl = index(a, br), index(a, bl)
    partner = me + 1 - 2 * core

    def remote(k, p, src, dst, dev):
        return pltpu.make_async_remote_copy(
            src_ref=src, dst_ref=dst, send_sem=ssem.at[k, p], recv_sem=rsem.at[k, p],
            device_id={"sp": dev}, device_id_type=MESH)

    def sub(j, off=0, size=None):
        return (rows(a * DA + (j // 2) * DB + off, size or DB, 8), rows((j % 2) * CB, CB, 128))

    mine = core

    def d_u(p):
        return remote(0, p, usend.at[p % 2], ubuf.at[p % USLOTS, rows(core * S, S, 16)], partner)

    def d_a1(p):
        return (remote(1, p, hbuf.at[p, rows(ao * DA, DB, 8)], ra1.at[p, 0], dev_ar),
                remote(2, p, hbuf.at[p, rows(ao * DA + DB, DB, 8)], ra1.at[p, 1], dev_al))

    def d_a2(p):
        return (remote(3, p, hbuf.at[p, rows(ar * DA, DA, 8)], ra2.at[p, 0], dev_ar),
                remote(4, p, hbuf.at[p, rows(al * DA, DA, 8)], ra2.at[p, 1], dev_al))

    def d_b1(p):
        return (remote(5, p, hbuf.at[(p, *sub(bo, 0, DB // 2))], rb1.at[p, 0], dev_br),
                remote(6, p, hbuf.at[(p, *sub(bo, DB // 2, DB // 2))], rb1.at[p, 1], dev_bl))

    def d_b2(p):
        return (remote(7, p, hbuf.at[(p, *sub(br))], rb2.at[p, 0], dev_br),
                remote(8, p, hbuf.at[(p, *sub(bl))], rb2.at[p, 1], dev_bl))

    def d_g1(p):
        here = gbuf.at[(p, mine, *sub(b))]
        return remote(9, p, here, here, dev_br), remote(10, p, here, here, dev_bl)

    def d_g2(p):
        top = gbuf.at[(p, mine, *sub(bl, 0, 32))]
        bottom = gbuf.at[(p, mine, *sub(br, 32, DB - 32))]
        return remote(11, p, top, top, dev_br), remote(12, p, bottom, bottom, dev_bl)

    def d_g3(p):
        here = gbuf.at[p, mine, rows(a * DA, DA, 16)]
        return remote(13, p, here, here, dev_ar), remote(14, p, here, here, dev_al)

    def d_g4(p):
        top = gbuf.at[p, mine, rows(al * DA, DB, 16)]
        bottom = gbuf.at[p, mine, rows(ar * DA + DB, DB, 16)]
        return remote(15, p, top, top, dev_ar), remote(16, p, bottom, bottom, dev_al)

    def d_g5(p):
        here = gbuf.at[p, mine]
        return remote(17, p, here, here, partner)

    def d_x(p):
        return (pltpu.make_async_copy(x_hbm.at[2 * p + 1 - core], xbuf.at[p % 2, 0], xsem.at[p % 2, 0]),
                pltpu.make_async_copy(x_hbm.at[2 * p + core], xbuf.at[p % 2, 1], xsem.at[p % 2, 1]))

    def d_out(p):
        return pltpu.make_async_copy(gbuf.at[p], g_out.at[p - done_pairs], osem.at[p - done_pairs])

    wt1 = ubuf.at[USLOTS - 1, :, pl.ds(0, D)] if D <= C else None
    ch_copies = (pltpu.make_async_copy(w1_hbm, w1, wsem.at[3]), pltpu.make_async_copy(w2_hbm, w2, wsem.at[4]))
    w_copies = (pltpu.make_async_copy(wt1_hbm.at[rows(chip * 2 * S, 2 * S, 16)], wt1, wsem.at[0]),
                pltpu.make_async_copy(wt2_hbm.at[:, rows(me * S, S, 128)], wt2, wsem.at[1]),
                pltpu.make_async_copy(bt2_hbm.at[:, rows(me * S, S, 128)], bt2, wsem.at[2]))

    def start(ds):
        for d in ds:
            d.start()

    def wait_recv(ds):
        for d in ds:
            d.wait_recv()

    LT = min(S, 64)

    def ln1(p):
        @pl.when(p + 1 < pairs)
        def _():
            start(d_x(p + 1))

        other, own = d_x(p)
        other.wait()

        @pl.when(p >= 2)
        def _():
            d_u(p - 2).wait_send()

        @pl.loop(0, S // LT)
        def _(i):
            r = rows(i * LT, LT, LT)
            usend[p % 2, r, :] = layer_norm(xbuf[p % 2, 0, r, :].astype(jnp.float32), row(s1_ref), row(o1_ref))

        @pl.when(p >= USLOTS)
        def _():
            pl.semaphore_wait(credit, 1)

        d_u(p).start()
        own.wait()

        @pl.loop(0, S // LT)
        def _(i):
            r = rows(i * LT, LT, LT)
            ubuf[p % USLOTS, rows(core * S + i * LT, LT, LT), :] = layer_norm(
                xbuf[p % 2, 1, r, :].astype(jnp.float32), row(s1_ref), row(o1_ref))

    def mm1(p):
        d_u(p).wait_recv()
        hbuf[p] = dot(wt1t[...], ubuf[p % USLOTS])

        @pl.when(p + USLOTS < pairs)
        def _():
            pl.semaphore_signal(credit, inc=1, device_id={"sp": partner}, device_id_type=MESH)

    def a1(p):
        start(d_a1(p))

    def a2(p):
        wait_recv(d_a1(p))
        hbuf[p, rows(ar * DA, DB, 8), :] += ra1[p, 0]
        hbuf[p, rows(al * DA + DB, DB, 8), :] += ra1[p, 1]
        start(d_a2(p))

    def b1(p):
        wait_recv(d_a2(p))
        hbuf[p, rows(a * DA, DA, 8), :] += ra2[p, 0] + ra2[p, 1]
        start(d_b1(p))

    def b2(p):
        wait_recv(d_b1(p))
        hbuf[(p, *sub(br, 0, DB // 2))] += rb1[p, 0]
        hbuf[(p, *sub(bl, DB // 2, DB // 2))] += rb1[p, 1]
        start(d_b2(p))

    def g1(p):
        wait_recv(d_b2(p))
        h = hbuf[(p, *sub(b))] + (rb2[p, 0] + rb2[p, 1])
        bias = b1c[rows(a * DA + (b // 2) * DB, DB, 8), 0:1]
        r, c = sub(b)
        gbuf[p, mine, rows(a * DA + (b // 2) * DB, DB, 16), c] = gelu(h + bias).astype(jnp.bfloat16)
        start(d_g1(p))

    def g2(p):
        wait_recv(d_g1(p))
        start(d_g2(p))

    def g3(p):
        wait_recv(d_g2(p))
        start(d_g3(p))

    def g4(p):
        wait_recv(d_g3(p))
        start(d_g4(p))

    def g5(p):
        wait_recv(d_g4(p))
        d_g5(p).start()

    def g6(p):
        d_g5(p).wait_recv()

        @pl.when(p >= done_pairs)
        def _():
            d_out(p).start()

    plan = ((g6, G6[0], G6[1]), (g5, G5[0], G5[1]), (g4, G4[0], G4[1]), (g3, G3[0], G3[1]), (g2, G2[0], G2[1]),
            (g1, G1[0], G1[1]), (b2, B2[0], B2[1]), (b1, B1[0], B1[1]), (a2, A2[0], A2[1]), (a1, A1[0], A1[1]))

    def slot(t, parity=None):
        for n, (stage, first, later) in enumerate(plan):
            if parity is not None and (later - parity) % 2 and (first < FIRST or (first - parity) % 2):
                continue
            if parity is None and n == len(plan) - 1:
                prepare(t)
            q = t + PERIOD * pairs - later
            p = q // PERIOD - pairs
            late = (q % PERIOD == 0) & (p >= 1) & (p < pairs)

            @pl.when(late | (t == first))
            def _():
                stage(jnp.where(late, p, 0))

    def prepare(t):
        @pl.when((t >= 1) & (t <= pairs))
        def _():
            mm1(t - 1)

    def image_of(k):
        return core + (k % 2) * (1 - 2 * core)

    def d_res(k):
        return pltpu.make_async_copy(x_hbm.at[(k // 2) * 2 + image_of(k)], xres.at[k % 2], xrsem.at[k % 2])

    def d_done(k):
        return pltpu.make_async_copy(obuf.at[k % 2], out_hbm.at[(k // 2) * 2 + image_of(k)], obsem.at[k % 2])

    mlp = functools.partial(mlp_half, wt2t_ref, bt2c_ref, s2_ref, o2_ref, w1, c1_ref, w2, c2_ref, v_scr, q_scr, x1_scr, acc)

    start(w_copies)
    start(d_x(0))
    barrier = pltpu.get_barrier_semaphore()
    neighbours = (dev_ar, dev_al, dev_br, dev_bl, partner)
    for dev in neighbours:
        pl.semaphore_signal(barrier, inc=1, device_id={"sp": dev}, device_id_type=MESH)
    b1c[...] = jnp.transpose(jnp.broadcast_to(row(bt1_ref), (128, D)))
    for w in w_copies:
        w.wait()
    start(ch_copies)
    d_res(0).start()
    wt1t[...] = jnp.transpose(wt1[...])
    pl.semaphore_wait(barrier, len(neighbours))
    steps = 2 * done_pairs

    @pl.loop(0, FIRST)
    def _(t):
        slot(t)

        @pl.when(t < pairs)
        def _():
            ln1(t)

        @pl.when(t == 0)
        def _():
            wt2t_ref[...] = jnp.transpose(wt2[...])
            bt2c_ref[...] = jnp.transpose(jnp.broadcast_to(bt2[...], (128, S)))

    for w in ch_copies:
        w.wait()

    @pl.loop(0, steps)
    def _(k):
        slot(FIRST + 2 * k, FIRST % 2)

        @pl.when(k + 1 < steps)
        def _():
            d_res(k + 1).start()

        d_res(k).wait()
        mlp(0, xres.at[k % 2], gbuf.at[k // 2, image_of(k)], None)
        slot(FIRST + 2 * k + 1, (FIRST + 1) % 2)

        @pl.when(k >= 2)
        def _():
            d_done(k - 2).wait()

        mlp(1, None, None, obuf.at[k % 2])
        d_done(k).start()

    @pl.loop(FIRST + 2 * steps, G6[1] + PERIOD * (pairs - 1) + 1)
    def _(t):
        slot(t)

    d_done(steps - 2).wait()
    d_done(steps - 1).wait()
    for p in (pairs - 2, pairs - 1):
        d_u(p).wait_send()

    @pl.loop(0, pairs)
    def _(p):
        for make in (d_a1, d_a2, d_b1, d_b2, d_g1, d_g2, d_g3, d_g4):
            for d in make(p):
                d.wait_send()
        d_g5(p).wait_send()

    @pl.loop(done_pairs, pairs)
    def _(p):
        d_out(p).wait()


def mlp_half(wt2t, bt2c, s2, o2, w1, c1, w2, c2, v_scr, q_scr, x1_scr, acc, half, x, g, out):
    H, hc = w1.shape[1], q_scr.shape[2]
    steps = H // hc
    if half == 0:
        t = (dot(wt2t[...], g[...]) + bt2c[:, 0:1]).astype(jnp.bfloat16)
        x1 = (x[...].astype(jnp.float32) + t.astype(jnp.float32)).astype(jnp.bfloat16)
        x1_scr[...] = x1
        v_scr[...] = layer_norm(x1.astype(jnp.float32), row(s2), row(o2))
    for c in range(0, steps // 2) if half == 0 else range(steps // 2, steps + 1):
        if c < steps:
            h = pl.ds(c * hc, hc)
            q_scr[c % 2] = gelu(dot(v_scr[...], w1[:, h]) + row(c1, h)).astype(jnp.bfloat16)
        if c >= 1:
            part = dot(q_scr[(c - 1) % 2], w2[pl.ds((c - 1) * hc, hc), :])
            if c == 1:
                acc[...] = part + row(c2)
            elif c < steps:
                acc[...] += part
            else:
                out[...] = (x1_scr[...].astype(jnp.float32) + (acc[...] + part)).astype(jnp.bfloat16)


def mlp_scratch(S, C, H):
    hc = min(512, H // 2)
    return [pltpu.VMEM((S, C), jnp.bfloat16), pltpu.VMEM((2, S, hc), jnp.bfloat16),
            pltpu.VMEM((S, C), jnp.bfloat16), pltpu.VMEM((S, C), jnp.float32)]


def exchange(side, done_pairs, patches, s1, o1, w_tok1, b_tok1, w_tok2, b_tok2, s2, o2, w_ch1, b_ch1, w_ch2, b_ch2):
    B, S, C = patches.shape
    pairs = B // 2
    D, H = w_tok1.shape[1], w_ch1.shape[1]
    DA, DB, CB = D // side, D // side // 2, C // 2
    f32, bf16 = jnp.float32, jnp.bfloat16
    return pl.pallas_call(
        functools.partial(exchange_kernel, side, done_pairs),
        out_shape=(jax.ShapeDtypeStruct((2 * done_pairs, S, C), bf16),
                   jax.ShapeDtypeStruct((pairs - done_pairs, 2, D, C), bf16),
                   jax.ShapeDtypeStruct((S, D), bf16),
                   jax.ShapeDtypeStruct((S, 128), f32)),
        in_specs=[ANY, VMEM, VMEM, ANY, VMEM, ANY, ANY, VMEM, VMEM, ANY, VMEM, ANY, VMEM],
        out_specs=(ANY, ANY, VMEM, VMEM),
        scratch_shapes=[
            pltpu.VMEM((2, 2, S, C), bf16),
            pltpu.VMEM((2, S, C), bf16),
            pltpu.VMEM((USLOTS, 2 * S, C), bf16),
            pltpu.VMEM((pairs, D, C), f32),
            pltpu.VMEM((pairs, 2, DB, C), f32),
            pltpu.VMEM((pairs, 2, DA, C), f32),
            pltpu.VMEM((pairs, 2, DB // 2, CB), f32),
            pltpu.VMEM((pairs, 2, DB, CB), f32),
            pltpu.VMEM((pairs, 2, D, C), bf16),
            pltpu.VMEM((D, 2 * S), bf16),
            pltpu.VMEM((D, S), bf16),
            pltpu.VMEM((1, S), f32),
            pltpu.VMEM((D, 128), f32),
            pltpu.VMEM((C, H), bf16),
            pltpu.VMEM((H, C), bf16),
            pltpu.VMEM((2, S, C), bf16),
            pltpu.VMEM((2, S, C), bf16),
            *mlp_scratch(S, C, H),
            pltpu.SemaphoreType.DMA((18, pairs)),
            pltpu.SemaphoreType.DMA((18, pairs)),
            pltpu.SemaphoreType.DMA((2, 2)),
            pltpu.SemaphoreType.DMA((5,)),
            pltpu.SemaphoreType.DMA((pairs - done_pairs,)),
            pltpu.SemaphoreType.DMA((2,)),
            pltpu.SemaphoreType.DMA((2,)),
            pltpu.SemaphoreType.REGULAR,
        ],
        compiler_params=pltpu.CompilerParams(collective_id=0, has_side_effects=True, vmem_limit_bytes=67043328),
        name="exchange",
    )(patches, s1, o1, w_tok1, b_tok1, w_tok2, b_tok2, s2, o2, w_ch1, b_ch1, w_ch2, b_ch2)


def finish_kernel(x_hbm, early_hbm, g_hbm, wt2t, bt2c, s2, o2, w1_hbm, c1, w2_hbm, c2, out_hbm,
                  carry, xbuf, gbuf, obuf, w1, w2, v_scr, q_scr, x1_scr, acc, csem, dsem, xsem, gsem, osem, wsem):
    early, rest = carry.shape[0], xbuf.shape[0]
    w_copies = (pltpu.make_async_copy(w1_hbm, w1, wsem.at[0]), pltpu.make_async_copy(w2_hbm, w2, wsem.at[1]))
    xs = [pltpu.make_async_copy(x_hbm.at[early + i], xbuf.at[i], xsem.at[i]) for i in range(rest)]
    gs = [pltpu.make_async_copy(g_hbm.at[i // 2, i % 2], gbuf.at[i], gsem.at[i]) for i in range(rest)]
    outs = [pltpu.make_async_copy(obuf.at[i], out_hbm.at[early + i], osem.at[i]) for i in range(rest)]
    ins = [pltpu.make_async_copy(early_hbm.at[i], carry.at[i], csem.at[i]) for i in range(early)]
    backs = [pltpu.make_async_copy(carry.at[i], out_hbm.at[i], dsem.at[i]) for i in range(early)]
    for i in range(rest):
        xs[i].start()
        gs[i].start()
        if i == 0:
            w_copies[0].start()
            w_copies[1].start()
    for c in ins:
        c.start()
    mlp = functools.partial(mlp_half, wt2t, bt2c, s2, o2, w1, c1, w2, c2, v_scr, q_scr, x1_scr, acc)
    for i in range(rest):
        xs[i].wait()
        gs[i].wait()
        if i == 0:
            w_copies[0].wait()
            w_copies[1].wait()
        mlp(0, xbuf.at[i], gbuf.at[i], None)
        if i == 0:
            for c, d in zip(ins, backs):
                c.wait()
                d.start()
        mlp(1, None, None, obuf.at[i])
        outs[i].start()
    for c in (*backs, *outs):
        c.wait()


def finish(patches, early, g, wt2t, bt2c, s2, o2, w_ch1, b_ch1, w_ch2, b_ch2):
    B, S, C = patches.shape
    D, H = g.shape[2], w_ch1.shape[1]
    n, rest = early.shape[0], B - early.shape[0]
    bf16 = jnp.bfloat16
    dma = pltpu.SemaphoreType.DMA
    return pl.pallas_call(
        finish_kernel,
        in_specs=[ANY, ANY, ANY, VMEM, VMEM, VMEM, VMEM, ANY, VMEM, ANY, VMEM],
        out_specs=ANY,
        out_shape=jax.ShapeDtypeStruct((B, S, C), bf16),
        scratch_shapes=[pltpu.VMEM((n, S, C), bf16), pltpu.VMEM((rest, S, C), bf16), pltpu.VMEM((rest, D, C), bf16),
                        pltpu.VMEM((rest, S, C), bf16), pltpu.VMEM((C, H), bf16), pltpu.VMEM((H, C), bf16),
                        *mlp_scratch(S, C, H), dma((n,)), dma((n,)), dma((rest,)), dma((rest,)), dma((rest,)), dma((2,))],
        compiler_params=pltpu.CompilerParams(vmem_limit_bytes=60 << 20),
        name="finish",
    )(patches, early, g, wt2t, bt2c, s2, o2, w_ch1, b_ch1, w_ch2, b_ch2)


def solution(mesh):
    row_spec = P('dp', 'sp', None)
    side = math.isqrt(mesh.shape['sp'] // 2)

    def local_layer(patches, ln1_scale, ln1_bias, w_tok1, b_tok1, w_tok2, b_tok2, ln2_scale, ln2_bias, w_ch1, b_ch1, w_ch2, b_ch2):
        tail = (ln2_scale, ln2_bias, w_ch1, b_ch1, w_ch2, b_ch2)
        early, g, wt2t, bt2c = exchange(side, patches.shape[0] // 2 - 1, patches, ln1_scale, ln1_bias, w_tok1, b_tok1,
                                        w_tok2, b_tok2[None], *tail)
        return finish(patches, early, g, wt2t, bt2c, *tail)

    return jax.shard_map(local_layer, mesh=mesh, in_specs=(row_spec,) + (P(),) * 12, out_specs=row_spec, check_vma=False)
```

```python
import functools
import math

import jax
import jax.numpy as jnp
from jax import lax
from jax.experimental import pallas as pl
from jax.experimental.pallas import tpu as pltpu
from jax.sharding import PartitionSpec as P

LN_EPS = 1e-6
K0 = math.sqrt(2.0 / math.pi)
K1 = K0 * 0.044715
MESH = pl.DeviceIdType.MESH
ANY = pl.BlockSpec(memory_space=pl.ANY)
VMEM = pl.BlockSpec(memory_space=pltpu.VMEM)
USLOTS = 4
FIRST, PERIOD = 7, 4
A1, A2, B1 = (None, 2, -5), (2, 4, -3), (3, 6, -1)
G1, G3, G4, G5, G6 = (4, 7, 1), (5, 8, 3), (6, 10, 5), (7, 11, 6), (9, 13, 7)


def layer_norm(rows_wide, scale, offset):
    mean = jnp.mean(rows_wide, axis=-1, keepdims=True)
    centered = rows_wide - mean
    var = jnp.mean(centered * centered, axis=-1, keepdims=True)
    return (centered * lax.rsqrt(var + LN_EPS) * scale + offset).astype(jnp.bfloat16)


def gelu(a):
    half = a * 0.5
    return half * jnp.tanh(a * ((a * a) * K1 + K0)) + half


def dot(a, b):
    return jnp.dot(a, b, preferred_element_type=jnp.float32)


def row(ref, cols=slice(None)):
    return ref[cols][None, :]


def rows(start, size, align):
    return pl.ds(pl.multiple_of(start, align), size)


def exchange_kernel(side, done_pairs, x_hbm, s1_ref, o1_ref, wt1_hbm, bt1_ref, wt2_hbm, bt2_hbm,
                    s2_ref, o2_ref, w1_hbm, c1_ref, w2_hbm, c2_ref,
                    out_hbm, g_out, wt2t_ref, bt2c_ref,
                    xbuf, usend, ubuf, hbuf, ra1, ra2, rb, gbuf, wt1t, wt2, bt2, b1c,
                    w1, w2, xres, obuf, v_scr, q_scr, x1_scr, acc,
                    ssem, rsem, xsem, wsem, osem, xrsem, obsem, credit):
    B, S, C = x_hbm.shape
    pairs = B // 2
    D = wt1_hbm.shape[1]
    DA, DB, CB = D // side, D // side // 2, C // 2

    me = lax.axis_index("sp")
    core = me % 2
    chip = me // 2
    cx, cy = chip % side, chip // side
    a = cx * (1 - core) + cy * core
    b = cy * (1 - core) + cx * core

    def index(ia, ib):
        ix = ia * (1 - core) + ib * core
        iy = ib * (1 - core) + ia * core
        return (iy * side + ix) * 2 + core

    ar, al, ao = (a + 1) % side, (a + side - 1) % side, (a + 2) % side
    br, bl, bo = (b + 1) % side, (b + side - 1) % side, (b + 2) % side
    dev_ar, dev_al = index(ar, b), index(al, b)
    dev_br, dev_bl, dev_bo = index(a, br), index(a, bl), index(a, bo)
    partner = me + 1 - 2 * core

    def remote(k, p, src, dst, dev):
        return pltpu.make_async_remote_copy(
            src_ref=src, dst_ref=dst, send_sem=ssem.at[k, p], recv_sem=rsem.at[k, p],
            device_id={"sp": dev}, device_id_type=MESH)

    def sub(j):
        return (rows(a * DA + (j // 2) * DB, DB, 16), rows((j % 2) * CB, CB, 128))

    mine = core

    def d_u(p):
        return remote(0, p, usend.at[p % 2], ubuf.at[p % USLOTS, rows(core * S, S, 16)], partner)

    def d_a1(p):
        return (remote(1, p, hbuf.at[p, rows(ao * DA, DB, 8)], ra1.at[p, 0], dev_ar),
                remote(2, p, hbuf.at[p, rows(ao * DA + DB, DB, 8)], ra1.at[p, 1], dev_al))

    def d_a2(p):
        return (remote(3, p, hbuf.at[p, rows(ar * DA, DA, 8)], ra2.at[p, 0], dev_ar),
                remote(4, p, hbuf.at[p, rows(al * DA, DA, 8)], ra2.at[p, 1], dev_al))

    def d_b1(p):
        return tuple(remote(5 + i, p, hbuf.at[(p, *sub(j))], rb.at[p, i], dev)
                     for i, (j, dev) in enumerate(((br, dev_br), (bl, dev_bl), (bo, dev_bo))))

    def d_g1(p):
        here = gbuf.at[(p, mine, *sub(b))]
        return tuple(remote(8 + i, p, here, here, dev) for i, dev in enumerate((dev_br, dev_bl, dev_bo)))

    def d_g3(p):
        here = gbuf.at[p, mine, rows(a * DA, DA, 16)]
        return remote(11, p, here, here, dev_ar), remote(12, p, here, here, dev_al)

    def d_g4(p):
        top = gbuf.at[p, mine, rows(al * DA, DB, 16)]
        bottom = gbuf.at[p, mine, rows(ar * DA + DB, DB, 16)]
        return remote(13, p, top, top, dev_ar), remote(14, p, bottom, bottom, dev_al)

    def d_g5(p):
        here = gbuf.at[p, mine]
        return remote(15, p, here, here, partner)

    def d_x(p):
        return (pltpu.make_async_copy(x_hbm.at[2 * p + 1 - core], xbuf.at[p % 2, 0], xsem.at[p % 2, 0]),
                pltpu.make_async_copy(x_hbm.at[2 * p + core], xbuf.at[p % 2, 1], xsem.at[p % 2, 1]))

    def d_out(p):
        return pltpu.make_async_copy(gbuf.at[p], g_out.at[p - done_pairs], osem.at[p - done_pairs])

    wt1 = ubuf.at[USLOTS - 1, :, pl.ds(0, D)] if D <= C else None
    ch_copies = (pltpu.make_async_copy(w1_hbm, w1, wsem.at[3]), pltpu.make_async_copy(w2_hbm, w2, wsem.at[4]))
    w_copies = (pltpu.make_async_copy(wt1_hbm.at[rows(chip * 2 * S, 2 * S, 16)], wt1, wsem.at[0]),
                pltpu.make_async_copy(wt2_hbm.at[:, rows(me * S, S, 128)], wt2, wsem.at[1]),
                pltpu.make_async_copy(bt2_hbm.at[:, rows(me * S, S, 128)], bt2, wsem.at[2]))

    def start(ds):
        for d in ds:
            d.start()

    def wait_recv(ds):
        for d in ds:
            d.wait_recv()

    LT = min(S, 256)

    def ln1(p):
        @pl.when(p + 1 < pairs)
        def _():
            start(d_x(p + 1))

        other, own = d_x(p)
        other.wait()

        @pl.when(p >= 2)
        def _():
            d_u(p - 2).wait_send()

        @pl.loop(0, S // LT)
        def _(i):
            r = rows(i * LT, LT, LT)
            usend[p % 2, r, :] = layer_norm(xbuf[p % 2, 0, r, :].astype(jnp.float32), row(s1_ref), row(o1_ref))

        @pl.when(p >= USLOTS)
        def _():
            pl.semaphore_wait(credit, 1)

        d_u(p).start()
        own.wait()

        @pl.loop(0, S // LT)
        def _(i):
            r = rows(i * LT, LT, LT)
            ubuf[p % USLOTS, rows(core * S + i * LT, LT, LT), :] = layer_norm(
                xbuf[p % 2, 1, r, :].astype(jnp.float32), row(s1_ref), row(o1_ref))

    def mm1(p):
        d_u(p).wait_recv()
        hbuf[p] = dot(wt1t[...], ubuf[p % USLOTS])

        @pl.when(p + USLOTS < pairs)
        def _():
            pl.semaphore_signal(credit, inc=1, device_id={"sp": partner}, device_id_type=MESH)

    def a1(p):
        start(d_a1(p))

    def a2(p):
        wait_recv(d_a1(p))
        hbuf[p, rows(ar * DA, DB, 8), :] += ra1[p, 0]
        hbuf[p, rows(al * DA + DB, DB, 8), :] += ra1[p, 1]
        start(d_a2(p))

    def b1(p):
        wait_recv(d_a2(p))
        hbuf[p, rows(a * DA, DA, 8), :] += ra2[p, 0] + ra2[p, 1]
        start(d_b1(p))

    def g1(p):
        wait_recv(d_b1(p))
        h = (hbuf[(p, *sub(b))] + rb[p, 2]) + (rb[p, 0] + rb[p, 1])
        r, c = sub(b)
        gbuf[p, mine, r, c] = gelu(h + b1c[r, 0:1]).astype(jnp.bfloat16)
        start(d_g1(p))

    def g3(p):
        wait_recv(d_g1(p))
        start(d_g3(p))

    def g4(p):
        wait_recv(d_g3(p))
        start(d_g4(p))

    def g5(p):
        wait_recv(d_g4(p))
        d_g5(p).start()

    def g6(p):
        d_g5(p).wait_recv()

        @pl.when(p >= done_pairs)
        def _():
            d_out(p).start()

    plan = ((g6, G6), (g5, G5), (g4, G4), (g3, G3), (g1, G1), (b1, B1), (a2, A2), (a1, A1))

    def slot(t, parity=None, lead=False):
        for stage, (first, second, later) in plan:
            if lead and stage is a1:
                prepare(t)
            firsts = [(p, u) for p, u in enumerate((first, second))
                      if u is not None and (lead == (u < FIRST)) and (lead or parity is None or (u - parity) % 2 == 0)]
            even = parity is None or (later - parity) % 2 == 0
            if not even and not firsts:
                continue
            due, pair = False, 0
            if even:
                q = t + PERIOD * pairs - later
                p = q // PERIOD - pairs
                due = (q % PERIOD == 0) & (p >= 2) & (p < pairs)
                pair = jnp.where(due, p, 0)
            for p, u in firsts:
                pair = pair + jnp.where(t == u, p, 0)
                due = due | (t == u)

            @pl.when(due)
            def _():
                stage(pair)

    def prepare(t):
        @pl.loop(0, 2)
        def _(j):
            p = 2 * t - 2 + j

            @pl.when((p >= 0) & (p < pairs))
            def _():
                mm1(p)

            @pl.when(p == 0)
            def _():
                a1(p)

    def image_of(k):
        return core + (k % 2) * (1 - 2 * core)

    def d_res(k):
        return pltpu.make_async_copy(x_hbm.at[(k // 2) * 2 + image_of(k)], xres.at[k % 2], xrsem.at[k % 2])

    def d_done(k):
        return pltpu.make_async_copy(obuf.at[k % 2], out_hbm.at[(k // 2) * 2 + image_of(k)], obsem.at[k % 2])

    mlp = functools.partial(mlp_half, wt2t_ref, bt2c_ref, s2_ref, o2_ref, w1, c1_ref, w2, c2_ref, v_scr, q_scr, x1_scr, acc)

    start(w_copies)
    start(d_x(0))
    barrier = pltpu.get_barrier_semaphore()
    neighbours = (dev_ar, dev_al, dev_br, dev_bl, dev_bo, partner)
    for dev in neighbours:
        pl.semaphore_signal(barrier, inc=1, device_id={"sp": dev}, device_id_type=MESH)
    b1c[...] = jnp.transpose(jnp.broadcast_to(row(bt1_ref), (128, D)))
    for w in w_copies:
        w.wait()
    start(ch_copies)
    d_res(0).start()
    wt1t[...] = jnp.transpose(wt1[...])
    pl.semaphore_wait(barrier, len(neighbours))
    steps = 2 * done_pairs

    @pl.loop(0, FIRST)
    def _(t):
        slot(t, lead=True)

        @pl.loop(0, 2)
        def _(j):
            @pl.when(2 * t + j < pairs)
            def _():
                ln1(2 * t + j)

        @pl.when(t == 0)
        def _():
            wt2t_ref[...] = jnp.transpose(wt2[...])
            bt2c_ref[...] = jnp.transpose(jnp.broadcast_to(bt2[...], (128, S)))

    for w in ch_copies:
        w.wait()

    @pl.loop(0, steps)
    def _(k):
        slot(FIRST + 2 * k, FIRST % 2)

        @pl.when(k + 1 < steps)
        def _():
            d_res(k + 1).start()

        d_res(k).wait()
        mlp(0, xres.at[k % 2], gbuf.at[k // 2, image_of(k)], None)
        slot(FIRST + 2 * k + 1, (FIRST + 1) % 2)

        @pl.when(k >= 2)
        def _():
            d_done(k - 2).wait()

        mlp(1, None, None, obuf.at[k % 2])
        d_done(k).start()

    @pl.loop(FIRST + 2 * steps, G6[2] + PERIOD * (pairs - 1) + 1)
    def _(t):
        slot(t)

    d_done(steps - 2).wait()
    d_done(steps - 1).wait()
    for p in (pairs - 2, pairs - 1):
        d_u(p).wait_send()

    @pl.loop(0, pairs)
    def _(p):
        for make in (d_a1, d_a2, d_b1, d_g1, d_g3, d_g4):
            for d in make(p):
                d.wait_send()
        d_g5(p).wait_send()

    @pl.loop(done_pairs, pairs)
    def _(p):
        d_out(p).wait()


def mlp_half(wt2t, bt2c, s2, o2, w1, c1, w2, c2, v_scr, q_scr, x1_scr, acc, half, x, g, out, ready=None):
    H, hc = w1.shape[1], q_scr.shape[2]
    steps = H // hc
    if half == 0:
        t = (dot(wt2t[...], g[...]) + bt2c[:, 0:1]).astype(jnp.bfloat16)
        x1 = (x[...].astype(jnp.float32) + t.astype(jnp.float32)).astype(jnp.bfloat16)
        x1_scr[...] = x1
        v_scr[...] = layer_norm(x1.astype(jnp.float32), row(s2), row(o2))
    for c in range(0, steps // 2) if half == 0 else range(steps // 2, steps + 1):
        if c < steps:
            h = pl.ds(c * hc, hc)
            if ready is not None:
                ready(c)
            q_scr[c % 2] = gelu(dot(v_scr[...], w1[:, h]) + row(c1, h)).astype(jnp.bfloat16)
        if c >= 1:
            part = dot(q_scr[(c - 1) % 2], w2[pl.ds((c - 1) * hc, hc), :])
            if c == 1:
                acc[...] = part + row(c2)
            elif c < steps:
                acc[...] += part
            else:
                out[...] = (x1_scr[...].astype(jnp.float32) + (acc[...] + part)).astype(jnp.bfloat16)


def mlp_scratch(S, C, H):
    hc = min(512, H // 2)
    return [pltpu.VMEM((S, C), jnp.bfloat16), pltpu.VMEM((2, S, hc), jnp.bfloat16),
            pltpu.VMEM((S, C), jnp.bfloat16), pltpu.VMEM((S, C), jnp.float32)]


def exchange(side, done_pairs, patches, s1, o1, w_tok1, b_tok1, w_tok2, b_tok2, s2, o2, w_ch1, b_ch1, w_ch2, b_ch2):
    B, S, C = patches.shape
    pairs = B // 2
    D, H = w_tok1.shape[1], w_ch1.shape[1]
    DA, DB, CB = D // side, D // side // 2, C // 2
    f32, bf16 = jnp.float32, jnp.bfloat16
    return pl.pallas_call(
        functools.partial(exchange_kernel, side, done_pairs),
        out_shape=(jax.ShapeDtypeStruct((2 * done_pairs, S, C), bf16),
                   jax.ShapeDtypeStruct((pairs - done_pairs, 2, D, C), bf16),
                   jax.ShapeDtypeStruct((S, D), bf16),
                   jax.ShapeDtypeStruct((S, 128), f32)),
        in_specs=[ANY, VMEM, VMEM, ANY, VMEM, ANY, ANY, VMEM, VMEM, ANY, VMEM, ANY, VMEM],
        out_specs=(ANY, ANY, VMEM, VMEM),
        scratch_shapes=[
            pltpu.VMEM((2, 2, S, C), bf16),
            pltpu.VMEM((2, S, C), bf16),
            pltpu.VMEM((USLOTS, 2 * S, C), bf16),
            pltpu.VMEM((pairs, D, C), f32),
            pltpu.VMEM((pairs, 2, DB, C), f32),
            pltpu.VMEM((pairs, 2, DA, C), f32),
            pltpu.VMEM((pairs, 3, DB, CB), f32),
            pltpu.VMEM((pairs, 2, D, C), bf16),
            pltpu.VMEM((D, 2 * S), bf16),
            pltpu.VMEM((D, S), bf16),
            pltpu.VMEM((1, S), f32),
            pltpu.VMEM((D, 128), f32),
            pltpu.VMEM((C, H), bf16),
            pltpu.VMEM((H, C), bf16),
            pltpu.VMEM((2, S, C), bf16),
            pltpu.VMEM((2, S, C), bf16),
            *mlp_scratch(S, C, H),
            pltpu.SemaphoreType.DMA((16, pairs)),
            pltpu.SemaphoreType.DMA((16, pairs)),
            pltpu.SemaphoreType.DMA((2, 2)),
            pltpu.SemaphoreType.DMA((5,)),
            pltpu.SemaphoreType.DMA((pairs - done_pairs,)),
            pltpu.SemaphoreType.DMA((2,)),
            pltpu.SemaphoreType.DMA((2,)),
            pltpu.SemaphoreType.REGULAR,
        ],
        compiler_params=pltpu.CompilerParams(collective_id=0, has_side_effects=True, vmem_limit_bytes=67043328),
        name="exchange",
    )(patches, s1, o1, w_tok1, b_tok1, w_tok2, b_tok2, s2, o2, w_ch1, b_ch1, w_ch2, b_ch2)


def finish_kernel(x_hbm, early_hbm, g_hbm, wt2t, bt2c, s2, o2, w1_hbm, c1, w2_hbm, c2, out_hbm,
                  carry, xbuf, gbuf, obuf, w1, w2, v_scr, q_scr, x1_scr, acc, csem, dsem, xsem, gsem, osem, wsem):
    early, rest = carry.shape[0], xbuf.shape[0]
    hc = q_scr.shape[2]
    ws = []
    for c in range(w1.shape[1] // hc):
        h = pl.ds(c * hc, hc)
        ws.append((pltpu.make_async_copy(w1_hbm.at[:, h], w1.at[:, h], wsem.at[c, 0]),
                   pltpu.make_async_copy(w2_hbm.at[h, :], w2.at[h, :], wsem.at[c, 1])))
    xs = [pltpu.make_async_copy(x_hbm.at[early + i], xbuf.at[i], xsem.at[i]) for i in range(rest)]
    gs = [pltpu.make_async_copy(g_hbm.at[i // 2, i % 2], gbuf.at[i], gsem.at[i]) for i in range(rest)]
    outs = [pltpu.make_async_copy(obuf.at[i], out_hbm.at[early + i], osem.at[i]) for i in range(rest)]
    ins = [pltpu.make_async_copy(early_hbm.at[i], carry.at[i], csem.at[i]) for i in range(early)]
    backs = [pltpu.make_async_copy(carry.at[i], out_hbm.at[i], dsem.at[i]) for i in range(early)]
    xs[0].start()
    gs[0].start()
    for w in ws:
        w[0].start()
        w[1].start()
    for i in range(1, rest):
        xs[i].start()
        gs[i].start()

    def ready(c):
        ws[c][0].wait()
        ws[c][1].wait()

    mlp = functools.partial(mlp_half, wt2t, bt2c, s2, o2, w1, c1, w2, c2, v_scr, q_scr, x1_scr, acc)
    for i in range(rest):
        xs[i].wait()
        gs[i].wait()
        mlp(0, xbuf.at[i], gbuf.at[i], None, ready if i == 0 else None)
        if i == 0:
            for c in ins:
                c.start()
        mlp(1, None, None, obuf.at[i], ready if i == 0 else None)
        outs[i].start()
        if i == 0:
            for c, d in zip(ins, backs):
                c.wait()
                d.start()
    for c in (*backs, *outs):
        c.wait()


def finish(patches, early, g, wt2t, bt2c, s2, o2, w_ch1, b_ch1, w_ch2, b_ch2):
    B, S, C = patches.shape
    D, H = g.shape[2], w_ch1.shape[1]
    n, rest = early.shape[0], B - early.shape[0]
    bf16 = jnp.bfloat16
    dma = pltpu.SemaphoreType.DMA
    return pl.pallas_call(
        finish_kernel,
        in_specs=[ANY, ANY, ANY, VMEM, VMEM, VMEM, VMEM, ANY, VMEM, ANY, VMEM],
        out_specs=ANY,
        out_shape=jax.ShapeDtypeStruct((B, S, C), bf16),
        scratch_shapes=[pltpu.VMEM((n, S, C), bf16), pltpu.VMEM((rest, S, C), bf16), pltpu.VMEM((rest, D, C), bf16),
                        pltpu.VMEM((rest, S, C), bf16), pltpu.VMEM((C, H), bf16), pltpu.VMEM((H, C), bf16),
                        *mlp_scratch(S, C, H), dma((n,)), dma((n,)), dma((rest,)), dma((rest,)), dma((rest,)), dma((H // min(512, H // 2), 2))],
        compiler_params=pltpu.CompilerParams(vmem_limit_bytes=60 << 20),
        name="finish",
    )(patches, early, g, wt2t, bt2c, s2, o2, w_ch1, b_ch1, w_ch2, b_ch2)


def solution(mesh):
    row_spec = P('dp', 'sp', None)
    side = math.isqrt(mesh.shape['sp'] // 2)

    def local_layer(patches, ln1_scale, ln1_bias, w_tok1, b_tok1, w_tok2, b_tok2, ln2_scale, ln2_bias, w_ch1, b_ch1, w_ch2, b_ch2):
        tail = (ln2_scale, ln2_bias, w_ch1, b_ch1, w_ch2, b_ch2)
        early, g, wt2t, bt2c = exchange(side, patches.shape[0] // 2 - 1, patches, ln1_scale, ln1_bias, w_tok1, b_tok1,
                                        w_tok2, b_tok2[None], *tail)
        return finish(patches, early, g, wt2t, bt2c, *tail)

    return jax.shard_map(local_layer, mesh=mesh, in_specs=(row_spec,) + (P(),) * 12, out_specs=row_spec, check_vma=False)
```

```python
import functools
import math

import jax
import jax.numpy as jnp
from jax import lax
from jax.experimental import pallas as pl
from jax.experimental.pallas import tpu as pltpu
from jax.sharding import PartitionSpec as P

LN_EPS = 1e-6
K0 = math.sqrt(2.0 / math.pi)
K1 = K0 * 0.044715
MESH = pl.DeviceIdType.MESH
ANY = pl.BlockSpec(memory_space=pl.ANY)
VMEM = pl.BlockSpec(memory_space=pltpu.VMEM)
USLOTS = 4
FIRST, SHIFT = 8, 2
PERIOD = 1 << SHIFT
A1, A2, B1 = (None, None, -6), (2, 3, -4), (3, 5, -1)
G1, G3, G4, G5, G6 = (4, 6, 1), (5, 8, 3), (6, 9, 5), (7, 11, 7), (9, 13, 9)
XSLOTS = 4


def layer_norm(rows_wide, scale, offset):
    mean = jnp.mean(rows_wide, axis=-1, keepdims=True)
    centered = rows_wide - mean
    var = jnp.mean(centered * centered, axis=-1, keepdims=True)
    return (centered * lax.rsqrt(var + LN_EPS) * scale + offset).astype(jnp.bfloat16)


def gelu(a):
    half = a * 0.5
    return half * jnp.tanh(a * ((a * a) * K1 + K0)) + half


def dot(a, b):
    return jnp.dot(a, b, preferred_element_type=jnp.float32)


def row(ref, cols=slice(None)):
    return ref[cols][None, :]


def rows(start, size, align):
    return pl.ds(pl.multiple_of(start, align), size)


def exchange_kernel(side, done_pairs, x_hbm, s1_ref, o1_ref, wt1_hbm, bt1_ref, wt2_hbm, bt2_hbm,
                    s2_ref, o2_ref, w1_hbm, c1_ref, w2_hbm, c2_ref,
                    out_hbm, g_out, wt2t_ref, bt2c_ref,
                    xbuf, usend, ubuf, hbuf, ra1, ra2, rb, gbuf, wt1t, wt2, bt2, b1c,
                    w1, w2, xres, obuf, v_scr, q_scr, x1_scr, acc,
                    ssem, rsem, xsem, wsem, osem, xrsem, obsem, credit):
    B, S, C = x_hbm.shape
    pairs = B // 2
    D = wt1_hbm.shape[1]
    DA, DB, CB = D // side, D // side // 2, C // 2

    me = lax.axis_index("sp")
    core = me % 2
    chip = me // 2
    cx, cy = chip % side, chip // side
    a = cx * (1 - core) + cy * core
    b = cy * (1 - core) + cx * core

    def index(ia, ib):
        ix = ia * (1 - core) + ib * core
        iy = ib * (1 - core) + ia * core
        return (iy * side + ix) * 2 + core

    ar, al, ao = (a + 1) % side, (a + side - 1) % side, (a + 2) % side
    br, bl, bo = (b + 1) % side, (b + side - 1) % side, (b + 2) % side
    dev_ar, dev_al = index(ar, b), index(al, b)
    dev_br, dev_bl, dev_bo = index(a, br), index(a, bl), index(a, bo)
    partner = me + 1 - 2 * core

    def remote(k, p, src, dst, dev):
        return pltpu.make_async_remote_copy(
            src_ref=src, dst_ref=dst, send_sem=ssem.at[k, p], recv_sem=rsem.at[k, p],
            device_id={"sp": dev}, device_id_type=MESH)

    def sub(j):
        return (rows(a * DA + (j // 2) * DB, DB, 16), rows((j % 2) * CB, CB, 128))

    mine = core

    def d_u(p):
        return remote(0, p, usend.at[p & 1], ubuf.at[p & (USLOTS - 1), rows(core * S, S, 16)], partner)

    def d_a1(p):
        return (remote(1, p, hbuf.at[p, rows(ao * DA, DB, 8)], ra1.at[p, 0], dev_ar),
                remote(2, p, hbuf.at[p, rows(ao * DA + DB, DB, 8)], ra1.at[p, 1], dev_al))

    def d_a2(p):
        return (remote(3, p, hbuf.at[p, rows(ar * DA, DA, 8)], ra2.at[p, 0], dev_ar),
                remote(4, p, hbuf.at[p, rows(al * DA, DA, 8)], ra2.at[p, 1], dev_al))

    def d_b1(p):
        return tuple(remote(5 + i, p, hbuf.at[(p, *sub(j))], rb.at[p, i], dev)
                     for i, (j, dev) in enumerate(((br, dev_br), (bl, dev_bl), (bo, dev_bo))))

    def d_g1(p):
        here = gbuf.at[(p, mine, *sub(b))]
        return tuple(remote(8 + i, p, here, here, dev) for i, dev in enumerate((dev_br, dev_bl, dev_bo)))

    def d_g3(p):
        here = gbuf.at[p, mine, rows(a * DA, DA, 16)]
        return remote(11, p, here, here, dev_ar), remote(12, p, here, here, dev_al)

    def d_g4(p):
        top = gbuf.at[p, mine, rows(al * DA, DB, 16)]
        bottom = gbuf.at[p, mine, rows(ar * DA + DB, DB, 16)]
        return remote(13, p, top, top, dev_ar), remote(14, p, bottom, bottom, dev_al)

    def d_g5(p):
        here = gbuf.at[p, mine]
        return remote(15, p, here, here, partner)

    def d_x(p, own):
        image = 2 * p + (core if own else 1 - core)
        n = p & (XSLOTS - 1)
        return pltpu.make_async_copy(x_hbm.at[image], xbuf.at[n, own], xsem.at[n, own])

    def d_out(p):
        return pltpu.make_async_copy(gbuf.at[p], g_out.at[p - done_pairs], osem.at[p - done_pairs])

    wt1 = ubuf.at[USLOTS - 1, :, pl.ds(0, D)] if D <= C else None
    ch_copies = (pltpu.make_async_copy(w1_hbm, w1, wsem.at[3]), pltpu.make_async_copy(w2_hbm, w2, wsem.at[4]))
    w_copies = (pltpu.make_async_copy(wt1_hbm.at[rows(chip * 2 * S, 2 * S, 16)], wt1, wsem.at[0]),
                pltpu.make_async_copy(wt2_hbm.at[:, rows(me * S, S, 128)], wt2, wsem.at[1]),
                pltpu.make_async_copy(bt2_hbm.at[:, rows(me * S, S, 128)], bt2, wsem.at[2]))

    def start(ds):
        for d in ds:
            d.start()

    def wait_recv(ds):
        for d in ds:
            d.wait_recv()

    LT = min(S, 256)

    def normed(p, which, i):
        return layer_norm(xbuf[p & (XSLOTS - 1), which, rows(i * LT, LT, LT), :].astype(jnp.float32), row(s1_ref), row(o1_ref))

    def ln_other(p):
        d_x(p, 0).wait()

        @pl.when(p >= 2)
        def _():
            d_u(p - 2).wait_send()

        @pl.loop(0, S // LT)
        def _(i):
            usend[p & 1, rows(i * LT, LT, LT), :] = normed(p, 0, i)

    def ln1(p):
        @pl.when(p + XSLOTS - 1 < pairs)
        def _():
            start((d_x(p + XSLOTS - 1, 0), d_x(p + XSLOTS - 1, 1)))

        @pl.when(p > 0)
        def _():
            ln_other(p)

            @pl.when(p >= USLOTS)
            def _():
                pl.semaphore_wait(credit, 1)

            d_u(p).start()

        d_x(p, 1).wait()

        @pl.loop(0, S // LT)
        def _(i):
            ubuf[p & (USLOTS - 1), rows(core * S + i * LT, LT, LT), :] = normed(p, 1, i)

    def mm1(p):
        d_u(p).wait_recv()
        hbuf[p] = dot(wt1t[...], ubuf[p & (USLOTS - 1)])

        @pl.when(p + USLOTS < pairs)
        def _():
            pl.semaphore_signal(credit, inc=1, device_id={"sp": partner}, device_id_type=MESH)

    def a1(p):
        start(d_a1(p))

    def a2(p):
        wait_recv(d_a1(p))
        hbuf[p, rows(ar * DA, DB, 8), :] += ra1[p, 0]
        hbuf[p, rows(al * DA + DB, DB, 8), :] += ra1[p, 1]
        start(d_a2(p))

    def b1(p):
        wait_recv(d_a2(p))
        hbuf[p, rows(a * DA, DA, 8), :] += ra2[p, 0] + ra2[p, 1]
        start(d_b1(p))

    def g1(p):
        wait_recv(d_b1(p))
        h = (hbuf[(p, *sub(b))] + rb[p, 2]) + (rb[p, 0] + rb[p, 1])
        r, c = sub(b)
        gbuf[p, mine, r, c] = gelu(h + b1c[r, 0:1]).astype(jnp.bfloat16)
        start(d_g1(p))

    def g3(p):
        wait_recv(d_g1(p))
        start(d_g3(p))

    def g4(p):
        wait_recv(d_g3(p))
        start(d_g4(p))

    def g5(p):
        wait_recv(d_g4(p))
        d_g5(p).start()

    def g6(p):
        d_g5(p).wait_recv()

        @pl.when(p >= done_pairs)
        def _():
            d_out(p).start()

    plan = ((g6, G6), (g5, G5), (g4, G4), (g3, G3), (g1, G1), (b1, B1), (a2, A2), (a1, A1))

    def slot(t, parity=None, lead=False):
        for stage, (*fixed, later) in plan:
            if lead and stage is a1:
                prepare(t)
            firsts = [(p, u) for p, u in enumerate(fixed)
                      if u is not None and (lead == (u < FIRST)) and (lead or parity is None or (u - parity) % 2 == 0)]
            even = parity is None or (later - parity) % 2 == 0
            if not even and not firsts:
                continue
            due, pair = False, 0
            if even:
                q = t + PERIOD * pairs - later
                p = (q >> SHIFT) - pairs
                due = (q & (PERIOD - 1) == 0) & (p >= len(fixed)) & (p < pairs)
                pair = jnp.where(due, p, 0)
            for p, u in firsts:
                pair = pair + jnp.where(t == u, p, 0)
                due = due | (t == u)

            @pl.when(due)
            def _():
                stage(pair)

    def upto(t):
        return 2 + ((3 * t) >> 1)

    def prepare(t):
        @pl.loop(upto(t - 2), upto(t - 1))
        def _(p):
            @pl.when((p >= 0) & (p < pairs))
            def _():
                mm1(p)

                @pl.when(p < 2)
                def _():
                    a1(p)

    def image_of(k):
        return core + (k & 1) * (1 - 2 * core)

    def d_res(k):
        return pltpu.make_async_copy(x_hbm.at[(k >> 1) * 2 + image_of(k)], xres.at[k & 1], xrsem.at[k & 1])

    def d_done(k):
        return pltpu.make_async_copy(obuf.at[k & 1], out_hbm.at[(k >> 1) * 2 + image_of(k)], obsem.at[k & 1])

    pre, mlp = channel_mlp(wt2t_ref, bt2c_ref, s2_ref, o2_ref, w1, c1_ref, w2, c2_ref, v_scr, q_scr, x1_scr, acc)
    steps = 2 * done_pairs

    start((d_x(0, 0), d_x(0, 1)))
    barrier = pltpu.get_barrier_semaphore()
    neighbours = (dev_ar, dev_al, dev_br, dev_bl, dev_bo, partner)
    for dev in neighbours:
        pl.semaphore_signal(barrier, inc=1, device_id={"sp": dev}, device_id_type=MESH)
    start(w_copies)
    for p in range(1, XSLOTS - 1):
        start((d_x(p, 0), d_x(p, 1)))
    ln_other(0)
    pl.semaphore_wait(barrier, len(neighbours))
    d_u(0).start()
    b1c[...] = jnp.transpose(jnp.broadcast_to(row(bt1_ref), (128, D)))
    for w in w_copies:
        w.wait()
    wt1t[...] = jnp.transpose(wt1[...])
    start(ch_copies)
    d_res(0).start()

    @pl.loop(0, FIRST)
    def _(t):
        slot(t, lead=True)

        @pl.loop(upto(t - 1), upto(t))
        def _(p):
            @pl.when(p < pairs)
            def _():
                ln1(p)

        @pl.when(t == 0)
        def _():
            wt2t_ref[...] = jnp.transpose(wt2[...])
            bt2c_ref[...] = jnp.transpose(jnp.broadcast_to(bt2[...], (128, S)))

    for w in ch_copies:
        w.wait()
    d_res(0).wait()
    pre(0, xres.at[0], gbuf.at[0, image_of(0)])

    @pl.loop(0, steps)
    def _(k):
        slot(FIRST + 2 * k, FIRST % 2)

        @pl.when(k + 1 < steps)
        def _():
            d_res(k + 1).start()

        mlp(0, k & 1)
        slot(FIRST + 2 * k + 1, (FIRST + 1) % 2)

        @pl.when(k + 1 < steps)
        def _():
            d_res(k + 1).wait()

        @pl.when(k >= 2)
        def _():
            d_done(k - 2).wait()

        following = jnp.minimum(k + 1, steps - 1)
        mlp(1, k & 1, obuf.at[k & 1],
            lambda: pre((k + 1) & 1, xres.at[(k + 1) & 1], gbuf.at[following >> 1, image_of(following)]))
        d_done(k).start()

    @pl.loop(FIRST + 2 * steps, G6[-1] + PERIOD * (pairs - 1) + 1)
    def _(t):
        slot(t)

    d_done(steps - 2).wait()
    d_done(steps - 1).wait()
    for p in (pairs - 2, pairs - 1):
        d_u(p).wait_send()

    @pl.loop(0, pairs)
    def _(p):
        for make in (d_a1, d_a2, d_b1, d_g1, d_g3, d_g4):
            for d in make(p):
                d.wait_send()
        d_g5(p).wait_send()

    @pl.loop(done_pairs, pairs)
    def _(p):
        d_out(p).wait()


def channel_mlp(wt2t, bt2c, s2, o2, w1, c1, w2, c2, v_scr, q_scr, x1_scr, acc):
    H, hc = w1.shape[1], q_scr.shape[2]
    steps = H // hc

    def pre(i, x, g):
        t = (dot(wt2t[...], g[...]) + bt2c[:, 0:1]).astype(jnp.bfloat16)
        x1 = (x[...].astype(jnp.float32) + t.astype(jnp.float32)).astype(jnp.bfloat16)
        x1_scr[i] = x1
        v_scr[i] = layer_norm(x1.astype(jnp.float32), row(s2), row(o2))

    def half(which, i, out=None, beside=None, ready=None):
        for c in range(0, steps // 2) if which == 0 else range(steps // 2, steps + 1):
            if c < steps:
                h = pl.ds(c * hc, hc)
                if ready is not None:
                    ready(c)
                q_scr[c % 2] = gelu(dot(v_scr[i], w1[:, h]) + row(c1, h)).astype(jnp.bfloat16)
            if c >= 1:
                part = dot(q_scr[(c - 1) % 2], w2[pl.ds((c - 1) * hc, hc), :])
                if c == 1:
                    acc[...] = part + row(c2)
                elif c < steps:
                    acc[...] += part
                else:
                    out[...] = (x1_scr[i].astype(jnp.float32) + (acc[...] + part)).astype(jnp.bfloat16)
            if c == steps - 1 and beside is not None:
                beside()

    return pre, half


def mlp_scratch(S, C, H):
    hc = H // 4
    return [pltpu.VMEM((2, S, C), jnp.bfloat16), pltpu.VMEM((2, S, hc), jnp.bfloat16),
            pltpu.VMEM((2, S, C), jnp.bfloat16), pltpu.VMEM((S, C), jnp.float32)]


def exchange(side, done_pairs, patches, s1, o1, w_tok1, b_tok1, w_tok2, b_tok2, s2, o2, w_ch1, b_ch1, w_ch2, b_ch2):
    B, S, C = patches.shape
    pairs = B // 2
    D, H = w_tok1.shape[1], w_ch1.shape[1]
    DA, DB, CB = D // side, D // side // 2, C // 2
    f32, bf16 = jnp.float32, jnp.bfloat16
    return pl.pallas_call(
        functools.partial(exchange_kernel, side, done_pairs),
        out_shape=(jax.ShapeDtypeStruct((2 * done_pairs, S, C), bf16),
                   jax.ShapeDtypeStruct((pairs - done_pairs, 2, D, C), bf16),
                   jax.ShapeDtypeStruct((S, D), bf16),
                   jax.ShapeDtypeStruct((S, 128), f32)),
        in_specs=[ANY, VMEM, VMEM, ANY, VMEM, ANY, ANY, VMEM, VMEM, ANY, VMEM, ANY, VMEM],
        out_specs=(ANY, ANY, VMEM, VMEM),
        scratch_shapes=[
            pltpu.VMEM((XSLOTS, 2, S, C), bf16),
            pltpu.VMEM((2, S, C), bf16),
            pltpu.VMEM((USLOTS, 2 * S, C), bf16),
            pltpu.VMEM((pairs, D, C), f32),
            pltpu.VMEM((pairs, 2, DB, C), f32),
            pltpu.VMEM((pairs, 2, DA, C), f32),
            pltpu.VMEM((pairs, 3, DB, CB), f32),
            pltpu.VMEM((pairs, 2, D, C), bf16),
            pltpu.VMEM((D, 2 * S), bf16),
            pltpu.VMEM((D, S), bf16),
            pltpu.VMEM((1, S), f32),
            pltpu.VMEM((D, 128), f32),
            pltpu.VMEM((C, H), bf16),
            pltpu.VMEM((H, C), bf16),
            pltpu.VMEM((2, S, C), bf16),
            pltpu.VMEM((2, S, C), bf16),
            *mlp_scratch(S, C, H),
            pltpu.SemaphoreType.DMA((16, pairs)),
            pltpu.SemaphoreType.DMA((16, pairs)),
            pltpu.SemaphoreType.DMA((XSLOTS, 2)),
            pltpu.SemaphoreType.DMA((5,)),
            pltpu.SemaphoreType.DMA((pairs - done_pairs,)),
            pltpu.SemaphoreType.DMA((2,)),
            pltpu.SemaphoreType.DMA((2,)),
            pltpu.SemaphoreType.REGULAR,
        ],
        compiler_params=pltpu.CompilerParams(collective_id=0, has_side_effects=True, vmem_limit_bytes=67043328),
        name="exchange",
    )(patches, s1, o1, w_tok1, b_tok1, w_tok2, b_tok2, s2, o2, w_ch1, b_ch1, w_ch2, b_ch2)


def finish_kernel(x_hbm, early_hbm, g_hbm, wt2t_hbm, bt2c_hbm, s2, o2, w1_hbm, c1, w2_hbm, c2, out_hbm,
                  carry, xbuf, gbuf, obuf, wt2t, bt2c, w1, w2, v_scr, q_scr, x1_scr, acc, csem, dsem, xsem, gsem, osem, wsem, tsem):
    early, rest = carry.shape[0], xbuf.shape[0]
    hc = q_scr.shape[2]
    ws = []
    for c in range(w1.shape[1] // hc):
        h = pl.ds(c * hc, hc)
        ws.append((pltpu.make_async_copy(w1_hbm.at[:, h], w1.at[:, h], wsem.at[c, 0]),
                   pltpu.make_async_copy(w2_hbm.at[h, :], w2.at[h, :], wsem.at[c, 1])))
    xs = [pltpu.make_async_copy(x_hbm.at[early + i], xbuf.at[i], xsem.at[i]) for i in range(rest)]
    gs = [pltpu.make_async_copy(g_hbm.at[i // 2, i % 2], gbuf.at[i], gsem.at[i]) for i in range(rest)]
    outs = [pltpu.make_async_copy(obuf.at[i], out_hbm.at[early + i], osem.at[i]) for i in range(rest)]
    ins = [pltpu.make_async_copy(early_hbm.at[i], carry.at[i], csem.at[i]) for i in range(early)]
    backs = [pltpu.make_async_copy(carry.at[i], out_hbm.at[i], dsem.at[i]) for i in range(early)]
    ts = (pltpu.make_async_copy(wt2t_hbm, wt2t, tsem.at[0]), pltpu.make_async_copy(bt2c_hbm, bt2c, tsem.at[1]))
    first = (*ts, xs[0], gs[0])
    for c in first:
        c.start()
    for w in ws:
        w[0].start()
        w[1].start()
    for i in range(1, rest):
        xs[i].start()
        gs[i].start()

    def ready(c):
        ws[c][0].wait()
        ws[c][1].wait()

    def following(i):
        return lambda: pre(i & 1, xbuf.at[i], gbuf.at[i]) if i < rest else None

    pre, mlp = channel_mlp(wt2t, bt2c, s2, o2, w1, c1, w2, c2, v_scr, q_scr, x1_scr, acc)
    for c in first:
        c.wait()
    pre(0, xbuf.at[0], gbuf.at[0])
    for i in range(rest):
        mlp(0, i & 1, ready=ready if i == 0 else None)
        if i == 0:
            for c in ins:
                c.start()
        if i + 1 < rest:
            xs[i + 1].wait()
            gs[i + 1].wait()
        mlp(1, i & 1, obuf.at[i], following(i + 1), ready if i == 0 else None)
        outs[i].start()
        if i == 0:
            for c, d in zip(ins, backs):
                c.wait()
                d.start()
    for c in (*backs, *outs):
        c.wait()


def finish(patches, early, g, wt2t, bt2c, s2, o2, w_ch1, b_ch1, w_ch2, b_ch2):
    B, S, C = patches.shape
    D, H = g.shape[2], w_ch1.shape[1]
    n, rest = early.shape[0], B - early.shape[0]
    bf16 = jnp.bfloat16
    dma = pltpu.SemaphoreType.DMA
    return pl.pallas_call(
        finish_kernel,
        in_specs=[ANY, ANY, ANY, ANY, ANY, VMEM, VMEM, ANY, VMEM, ANY, VMEM],
        out_specs=ANY,
        out_shape=jax.ShapeDtypeStruct((B, S, C), bf16),
        scratch_shapes=[pltpu.VMEM((n, S, C), bf16), pltpu.VMEM((rest, S, C), bf16), pltpu.VMEM((rest, D, C), bf16),
                        pltpu.VMEM((rest, S, C), bf16), pltpu.VMEM((S, D), bf16), pltpu.VMEM((S, 128), jnp.float32),
                        pltpu.VMEM((C, H), bf16), pltpu.VMEM((H, C), bf16),
                        *mlp_scratch(S, C, H), dma((n,)), dma((n,)), dma((rest,)), dma((rest,)), dma((rest,)), dma((4, 2)), dma((2,))],
        compiler_params=pltpu.CompilerParams(vmem_limit_bytes=60 << 20),
        name="finish",
    )(patches, early, g, wt2t, bt2c, s2, o2, w_ch1, b_ch1, w_ch2, b_ch2)


def solution(mesh):
    row_spec = P('dp', 'sp', None)
    side = math.isqrt(mesh.shape['sp'] // 2)

    def local_layer(patches, ln1_scale, ln1_bias, w_tok1, b_tok1, w_tok2, b_tok2, ln2_scale, ln2_bias, w_ch1, b_ch1, w_ch2, b_ch2):
        tail = (ln2_scale, ln2_bias, w_ch1, b_ch1, w_ch2, b_ch2)
        early, g, wt2t, bt2c = exchange(side, patches.shape[0] // 2 - 1, patches, ln1_scale, ln1_bias, w_tok1, b_tok1,
                                        w_tok2, b_tok2[None], *tail)
        return finish(patches, early, g, wt2t, bt2c, *tail)

    return jax.shard_map(local_layer, mesh=mesh, in_specs=(row_spec,) + (P(),) * 12, out_specs=row_spec, check_vma=False)
```

```python
import functools
import math

import jax
import jax.numpy as jnp
from jax import lax
from jax.experimental import pallas as pl
from jax.experimental.pallas import tpu as pltpu
from jax.sharding import PartitionSpec as P

LN_EPS = 1e-6
K0 = math.sqrt(2.0 / math.pi)
K1 = K0 * 0.044715
MESH = pl.DeviceIdType.MESH
ANY = pl.BlockSpec(memory_space=pl.ANY)
VMEM = pl.BlockSpec(memory_space=pltpu.VMEM)
USLOTS = 4
FIRST, SHIFT = 8, 2
PERIOD = 1 << SHIFT
A1, A2, B1 = (None, None, -6), (2, 3, -4), (3, 5, -1)
G1, G3, G4, G5, G6 = (4, 6, 1), (5, 8, 3), (6, 9, 5), (7, 11, 7), (9, 13, 9)
XSLOTS = 4


def layer_norm(rows_wide, scale, offset):
    mean = jnp.mean(rows_wide, axis=-1, keepdims=True)
    centered = rows_wide - mean
    var = jnp.mean(centered * centered, axis=-1, keepdims=True)
    return (centered * lax.rsqrt(var + LN_EPS) * scale + offset).astype(jnp.bfloat16)


def gelu(a):
    half = a * 0.5
    return half * jnp.tanh(a * ((a * a) * K1 + K0)) + half


def dot(a, b):
    return jnp.dot(a, b, preferred_element_type=jnp.float32)


def row(ref, cols=slice(None)):
    return ref[cols][None, :]


def rows(start, size, align):
    return pl.ds(pl.multiple_of(start, align), size)


def exchange_kernel(side, done_pairs, x_hbm, s1_ref, o1_ref, wt1_hbm, bt1_ref, wt2_hbm, bt2_hbm,
                    s2_ref, o2_ref, w1_hbm, c1_ref, w2_hbm, c2_ref,
                    out_hbm, g_out, wt2t_out, bt2c_out,
                    xbuf, usend, ubuf, hbuf, ra1, ra2, rb, gbuf, wt1t, wt2, bt2, b1c,
                    w1, w2, wt2t_ref, bt2c_ref, xres, obuf, v_scr, q_scr, x1_scr, acc,
                    ssem, rsem, xsem, wsem, osem, xrsem, obsem, credit):
    B, S, C = x_hbm.shape
    pairs = B // 2
    D = wt1_hbm.shape[1]
    DA, DB, CB = D // side, D // side // 2, C // 2

    me = lax.axis_index("sp")
    core = me % 2
    chip = me // 2
    cx, cy = chip % side, chip // side
    a = cx * (1 - core) + cy * core
    b = cy * (1 - core) + cx * core

    def index(ia, ib):
        ix = ia * (1 - core) + ib * core
        iy = ib * (1 - core) + ia * core
        return (iy * side + ix) * 2 + core

    ar, al, ao = (a + 1) % side, (a + side - 1) % side, (a + 2) % side
    br, bl, bo = (b + 1) % side, (b + side - 1) % side, (b + 2) % side
    dev_ar, dev_al = index(ar, b), index(al, b)
    dev_br, dev_bl, dev_bo = index(a, br), index(a, bl), index(a, bo)
    partner = me + 1 - 2 * core

    def remote(k, p, src, dst, dev):
        return pltpu.make_async_remote_copy(
            src_ref=src, dst_ref=dst, send_sem=ssem.at[k, p], recv_sem=rsem.at[k, p],
            device_id={"sp": dev}, device_id_type=MESH)

    def sub(j):
        return (rows(a * DA + (j // 2) * DB, DB, 16), rows((j % 2) * CB, CB, 128))

    mine = core

    def d_u(p):
        return remote(0, p, usend.at[p & 1], ubuf.at[p & (USLOTS - 1), rows(core * S, S, 16)], partner)

    def d_a1(p):
        return (remote(1, p, hbuf.at[p, rows(ao * DA, DB, 8)], ra1.at[p, 0], dev_ar),
                remote(2, p, hbuf.at[p, rows(ao * DA + DB, DB, 8)], ra1.at[p, 1], dev_al))

    def d_a2(p):
        return (remote(3, p, hbuf.at[p, rows(ar * DA, DA, 8)], ra2.at[p, 0], dev_ar),
                remote(4, p, hbuf.at[p, rows(al * DA, DA, 8)], ra2.at[p, 1], dev_al))

    def d_b1(p):
        return tuple(remote(5 + i, p, hbuf.at[(p, *sub(j))], rb.at[p, i], dev)
                     for i, (j, dev) in enumerate(((br, dev_br), (bl, dev_bl), (bo, dev_bo))))

    def d_g1(p):
        here = gbuf.at[(p, mine, *sub(b))]
        return tuple(remote(8 + i, p, here, here, dev) for i, dev in enumerate((dev_br, dev_bl, dev_bo)))

    def d_g3(p):
        here = gbuf.at[p, mine, rows(a * DA, DA, 16)]
        return remote(11, p, here, here, dev_ar), remote(12, p, here, here, dev_al)

    def d_g4(p):
        top = gbuf.at[p, mine, rows(al * DA, DB, 16)]
        bottom = gbuf.at[p, mine, rows(ar * DA + DB, DB, 16)]
        return remote(13, p, top, top, dev_ar), remote(14, p, bottom, bottom, dev_al)

    def d_g5(p):
        here = gbuf.at[p, mine]
        return remote(15, p, here, here, partner)

    def d_x(p, own):
        image = 2 * p + (core if own else 1 - core)
        n = p & (XSLOTS - 1)
        return pltpu.make_async_copy(x_hbm.at[image], xbuf.at[n, own], xsem.at[n, own])

    def d_out(p):
        return pltpu.make_async_copy(gbuf.at[p], g_out.at[p - done_pairs], osem.at[p - done_pairs])

    wt1 = ubuf.at[USLOTS - 1, :, pl.ds(0, D)] if D <= C else None
    t_copies = (pltpu.make_async_copy(wt2t_ref, wt2t_out, wsem.at[5]), pltpu.make_async_copy(bt2c_ref, bt2c_out, wsem.at[6]))
    ch_copies = (pltpu.make_async_copy(w1_hbm, w1, wsem.at[3]), pltpu.make_async_copy(w2_hbm, w2, wsem.at[4]))
    w_copies = (pltpu.make_async_copy(wt1_hbm.at[rows(chip * 2 * S, 2 * S, 16)], wt1, wsem.at[0]),
                pltpu.make_async_copy(wt2_hbm.at[:, rows(me * S, S, 128)], wt2, wsem.at[1]),
                pltpu.make_async_copy(bt2_hbm.at[:, rows(me * S, S, 128)], bt2, wsem.at[2]))

    def start(ds):
        for d in ds:
            d.start()

    def wait_recv(ds):
        for d in ds:
            d.wait_recv()

    LT = min(S, 256)

    def normed(p, which, i):
        return layer_norm(xbuf[p & (XSLOTS - 1), which, rows(i * LT, LT, LT), :].astype(jnp.float32), row(s1_ref), row(o1_ref))

    def ln_other(p):
        d_x(p, 0).wait()

        @pl.when(p >= 2)
        def _():
            d_u(p - 2).wait_send()

        @pl.loop(0, S // LT)
        def _(i):
            usend[p & 1, rows(i * LT, LT, LT), :] = normed(p, 0, i)

    def ln1(p):
        @pl.when(p + XSLOTS - 1 < pairs)
        def _():
            start((d_x(p + XSLOTS - 1, 0), d_x(p + XSLOTS - 1, 1)))

        @pl.when(p > 0)
        def _():
            ln_other(p)

            @pl.when(p >= USLOTS)
            def _():
                pl.semaphore_wait(credit, 1)

            d_u(p).start()

        d_x(p, 1).wait()

        @pl.loop(0, S // LT)
        def _(i):
            ubuf[p & (USLOTS - 1), rows(core * S + i * LT, LT, LT), :] = normed(p, 1, i)

    def mm1(p):
        d_u(p).wait_recv()
        hbuf[p] = dot(wt1t[...], ubuf[p & (USLOTS - 1)])

        @pl.when(p + USLOTS < pairs)
        def _():
            pl.semaphore_signal(credit, inc=1, device_id={"sp": partner}, device_id_type=MESH)

    def a1(p):
        start(d_a1(p))

    def a2(p):
        wait_recv(d_a1(p))
        hbuf[p, rows(ar * DA, DB, 8), :] += ra1[p, 0]
        hbuf[p, rows(al * DA + DB, DB, 8), :] += ra1[p, 1]
        start(d_a2(p))

    def b1(p):
        wait_recv(d_a2(p))
        hbuf[p, rows(a * DA, DA, 8), :] += ra2[p, 0] + ra2[p, 1]
        start(d_b1(p))

    def g1(p):
        wait_recv(d_b1(p))
        h = (hbuf[(p, *sub(b))] + rb[p, 2]) + (rb[p, 0] + rb[p, 1])
        r, c = sub(b)
        gbuf[p, mine, r, c] = gelu(h + b1c[r, 0:1]).astype(jnp.bfloat16)
        start(d_g1(p))

    def g3(p):
        wait_recv(d_g1(p))
        start(d_g3(p))

    def g4(p):
        wait_recv(d_g3(p))
        start(d_g4(p))

    def g5(p):
        wait_recv(d_g4(p))
        d_g5(p).start()

    def g6(p):
        d_g5(p).wait_recv()

        @pl.when(p >= done_pairs)
        def _():
            d_out(p).start()

    plan = ((g6, G6), (g5, G5), (g4, G4), (g3, G3), (g1, G1), (b1, B1), (a2, A2), (a1, A1))

    def slot(t, parity=None, lead=False):
        for stage, (*fixed, later) in plan:
            if lead and stage is a1:
                prepare(t)
            firsts = [(p, u) for p, u in enumerate(fixed)
                      if u is not None and (lead == (u < FIRST)) and (lead or parity is None or (u - parity) % 2 == 0)]
            even = parity is None or (later - parity) % 2 == 0
            if not even and not firsts:
                continue
            due, pair = False, 0
            if even:
                q = t + PERIOD * pairs - later
                p = (q >> SHIFT) - pairs
                due = (q & (PERIOD - 1) == 0) & (p >= len(fixed)) & (p < pairs)
                pair = jnp.where(due, p, 0)
            for p, u in firsts:
                pair = pair + jnp.where(t == u, p, 0)
                due = due | (t == u)

            @pl.when(due)
            def _():
                stage(pair)

    def upto(t):
        return 2 + ((3 * t) >> 1)

    def prepare(t):
        @pl.loop(upto(t - 2), upto(t - 1))
        def _(p):
            @pl.when((p >= 0) & (p < pairs))
            def _():
                mm1(p)

                @pl.when(p < 2)
                def _():
                    a1(p)

    def image_of(k):
        return core + (k & 1) * (1 - 2 * core)

    def d_res(k):
        return pltpu.make_async_copy(x_hbm.at[(k >> 1) * 2 + image_of(k)], xres.at[k & 1], xrsem.at[k & 1])

    def d_done(k):
        return pltpu.make_async_copy(obuf.at[k & 1], out_hbm.at[(k >> 1) * 2 + image_of(k)], obsem.at[k & 1])

    pre, mlp = channel_mlp(wt2t_ref, bt2c_ref, s2_ref, o2_ref, w1, c1_ref, w2, c2_ref, v_scr, q_scr, x1_scr, acc)
    steps = 2 * done_pairs

    start((d_x(0, 0), d_x(0, 1)))
    barrier = pltpu.get_barrier_semaphore()
    neighbours = (dev_ar, dev_al, dev_br, dev_bl, dev_bo, partner)
    for dev in neighbours:
        pl.semaphore_signal(barrier, inc=1, device_id={"sp": dev}, device_id_type=MESH)
    start(w_copies)
    for p in range(1, XSLOTS - 1):
        start((d_x(p, 0), d_x(p, 1)))
    ln_other(0)
    pl.semaphore_wait(barrier, len(neighbours))
    d_u(0).start()
    b1c[...] = jnp.transpose(jnp.broadcast_to(row(bt1_ref), (128, D)))
    for w in w_copies:
        w.wait()
    wt1t[...] = jnp.transpose(wt1[...])
    start(ch_copies)
    d_res(0).start()

    @pl.loop(0, FIRST)
    def _(t):
        slot(t, lead=True)

        @pl.loop(upto(t - 1), upto(t))
        def _(p):
            @pl.when(p < pairs)
            def _():
                ln1(p)

        @pl.when(t == 0)
        def _():
            wt2t_ref[...] = jnp.transpose(wt2[...])
            bt2c_ref[...] = jnp.transpose(jnp.broadcast_to(bt2[...], (128, S)))

    start(t_copies)
    for w in ch_copies:
        w.wait()
    d_res(0).wait()
    pre(0, xres.at[0], gbuf.at[0, image_of(0)])

    @pl.loop(0, steps)
    def _(k):
        slot(FIRST + 2 * k, FIRST % 2)

        @pl.when(k + 1 < steps)
        def _():
            d_res(k + 1).start()

        mlp(0, k & 1)
        slot(FIRST + 2 * k + 1, (FIRST + 1) % 2)

        @pl.when(k + 1 < steps)
        def _():
            d_res(k + 1).wait()

        @pl.when(k >= 2)
        def _():
            d_done(k - 2).wait()

        following = jnp.minimum(k + 1, steps - 1)
        mlp(1, k & 1, obuf.at[k & 1],
            lambda: pre((k + 1) & 1, xres.at[(k + 1) & 1], gbuf.at[following >> 1, image_of(following)]))
        d_done(k).start()

    @pl.loop(FIRST + 2 * steps, G6[-1] + PERIOD * (pairs - 1) + 1)
    def _(t):
        slot(t)

    d_done(steps - 2).wait()
    d_done(steps - 1).wait()
    for w in t_copies:
        w.wait()
    for p in (pairs - 2, pairs - 1):
        d_u(p).wait_send()

    @pl.loop(0, pairs)
    def _(p):
        for make in (d_a1, d_a2, d_b1, d_g1, d_g3, d_g4):
            for d in make(p):
                d.wait_send()
        d_g5(p).wait_send()

    @pl.loop(done_pairs, pairs)
    def _(p):
        d_out(p).wait()


def channel_mlp(wt2t, bt2c, s2, o2, w1, c1, w2, c2, v_scr, q_scr, x1_scr, acc):
    H, hc = w1.shape[1], q_scr.shape[2]
    steps = H // hc

    def pre(i, x, g):
        t = (dot(wt2t[...], g[...]) + bt2c[:, 0:1]).astype(jnp.bfloat16)
        x1 = (x[...].astype(jnp.float32) + t.astype(jnp.float32)).astype(jnp.bfloat16)
        x1_scr[i] = x1
        v_scr[i] = layer_norm(x1.astype(jnp.float32), row(s2), row(o2))

    def half(which, i, out=None, beside=None, ready=None):
        for c in range(0, steps // 2) if which == 0 else range(steps // 2, steps + 1):
            if c < steps:
                h = pl.ds(c * hc, hc)
                if ready is not None:
                    ready(c)
                q_scr[c % 2] = gelu(dot(v_scr[i], w1[:, h]) + row(c1, h)).astype(jnp.bfloat16)
            if c >= 1:
                part = dot(q_scr[(c - 1) % 2], w2[pl.ds((c - 1) * hc, hc), :])
                if c == 1:
                    acc[...] = part + row(c2)
                elif c < steps:
                    acc[...] += part
                else:
                    out[...] = (x1_scr[i].astype(jnp.float32) + (acc[...] + part)).astype(jnp.bfloat16)
            if c == steps - 1 and beside is not None:
                beside()

    return pre, half


def mlp_scratch(S, C, H):
    hc = H // 4
    return [pltpu.VMEM((2, S, C), jnp.bfloat16), pltpu.VMEM((2, S, hc), jnp.bfloat16),
            pltpu.VMEM((2, S, C), jnp.bfloat16), pltpu.VMEM((S, C), jnp.float32)]


def exchange(side, done_pairs, patches, s1, o1, w_tok1, b_tok1, w_tok2, b_tok2, s2, o2, w_ch1, b_ch1, w_ch2, b_ch2):
    B, S, C = patches.shape
    pairs = B // 2
    D, H = w_tok1.shape[1], w_ch1.shape[1]
    DA, DB, CB = D // side, D // side // 2, C // 2
    f32, bf16 = jnp.float32, jnp.bfloat16
    return pl.pallas_call(
        functools.partial(exchange_kernel, side, done_pairs),
        out_shape=(jax.ShapeDtypeStruct((2 * done_pairs, S, C), bf16),
                   jax.ShapeDtypeStruct((pairs - done_pairs, 2, D, C), bf16),
                   jax.ShapeDtypeStruct((S, D), bf16),
                   jax.ShapeDtypeStruct((S, 128), f32)),
        in_specs=[ANY, VMEM, VMEM, ANY, VMEM, ANY, ANY, VMEM, VMEM, ANY, VMEM, ANY, VMEM],
        out_specs=(ANY, ANY, ANY, ANY),
        scratch_shapes=[
            pltpu.VMEM((XSLOTS, 2, S, C), bf16),
            pltpu.VMEM((2, S, C), bf16),
            pltpu.VMEM((USLOTS, 2 * S, C), bf16),
            pltpu.VMEM((pairs, D, C), f32),
            pltpu.VMEM((pairs, 2, DB, C), f32),
            pltpu.VMEM((pairs, 2, DA, C), f32),
            pltpu.VMEM((pairs, 3, DB, CB), f32),
            pltpu.VMEM((pairs, 2, D, C), bf16),
            pltpu.VMEM((D, 2 * S), bf16),
            pltpu.VMEM((D, S), bf16),
            pltpu.VMEM((1, S), f32),
            pltpu.VMEM((D, 128), f32),
            pltpu.VMEM((C, H), bf16),
            pltpu.VMEM((H, C), bf16),
            pltpu.VMEM((S, D), bf16),
            pltpu.VMEM((S, 128), f32),
            pltpu.VMEM((2, S, C), bf16),
            pltpu.VMEM((2, S, C), bf16),
            *mlp_scratch(S, C, H),
            pltpu.SemaphoreType.DMA((16, pairs)),
            pltpu.SemaphoreType.DMA((16, pairs)),
            pltpu.SemaphoreType.DMA((XSLOTS, 2)),
            pltpu.SemaphoreType.DMA((7,)),
            pltpu.SemaphoreType.DMA((pairs - done_pairs,)),
            pltpu.SemaphoreType.DMA((2,)),
            pltpu.SemaphoreType.DMA((2,)),
            pltpu.SemaphoreType.REGULAR,
        ],
        compiler_params=pltpu.CompilerParams(collective_id=0, has_side_effects=True, vmem_limit_bytes=67043328),
        name="exchange",
    )(patches, s1, o1, w_tok1, b_tok1, w_tok2, b_tok2, s2, o2, w_ch1, b_ch1, w_ch2, b_ch2)


def finish_kernel(x_hbm, early_hbm, g_hbm, wt2t_hbm, bt2c_hbm, s2, o2, w1_hbm, c1, w2_hbm, c2, out_hbm,
                  carry, xbuf, gbuf, obuf, wt2t, bt2c, w1, w2, v_scr, q_scr, x1_scr, acc, csem, dsem, xsem, gsem, osem, wsem, tsem):
    early, rest = carry.shape[0], xbuf.shape[0]
    hc = q_scr.shape[2]
    ws = []
    for c in range(w1.shape[1] // hc):
        h = pl.ds(c * hc, hc)
        ws.append((pltpu.make_async_copy(w1_hbm.at[:, h], w1.at[:, h], wsem.at[c, 0]),
                   pltpu.make_async_copy(w2_hbm.at[h, :], w2.at[h, :], wsem.at[c, 1])))
    xs = [pltpu.make_async_copy(x_hbm.at[early + i], xbuf.at[i], xsem.at[i]) for i in range(rest)]
    gs = [pltpu.make_async_copy(g_hbm.at[i // 2, i % 2], gbuf.at[i], gsem.at[i]) for i in range(rest)]
    outs = [pltpu.make_async_copy(obuf.at[i], out_hbm.at[early + i], osem.at[i]) for i in range(rest)]
    ins = [pltpu.make_async_copy(early_hbm.at[i], carry.at[i], csem.at[i]) for i in range(early)]
    backs = [pltpu.make_async_copy(carry.at[i], out_hbm.at[i], dsem.at[i]) for i in range(early)]
    ts = (pltpu.make_async_copy(wt2t_hbm, wt2t, tsem.at[0]), pltpu.make_async_copy(bt2c_hbm, bt2c, tsem.at[1]))
    first = (*ts, xs[0], gs[0])
    for c in first:
        c.start()
    for w in ws:
        w[0].start()
        w[1].start()
    for i in range(1, rest):
        xs[i].start()
        gs[i].start()

    def ready(c):
        ws[c][0].wait()
        ws[c][1].wait()

    def following(i):
        return lambda: pre(i & 1, xbuf.at[i], gbuf.at[i]) if i < rest else None

    pre, mlp = channel_mlp(wt2t, bt2c, s2, o2, w1, c1, w2, c2, v_scr, q_scr, x1_scr, acc)
    for c in first:
        c.wait()
    pre(0, xbuf.at[0], gbuf.at[0])
    for i in range(rest):
        mlp(0, i & 1, ready=ready if i == 0 else None)
        if i == 0:
            for c in ins:
                c.start()
        if i + 1 < rest:
            xs[i + 1].wait()
            gs[i + 1].wait()
        mlp(1, i & 1, obuf.at[i], following(i + 1), ready if i == 0 else None)
        outs[i].start()
        if i == 0:
            for c, d in zip(ins, backs):
                c.wait()
                d.start()
    for c in (*backs, *outs):
        c.wait()


def finish(patches, early, g, wt2t, bt2c, s2, o2, w_ch1, b_ch1, w_ch2, b_ch2):
    B, S, C = patches.shape
    D, H = g.shape[2], w_ch1.shape[1]
    n, rest = early.shape[0], B - early.shape[0]
    bf16 = jnp.bfloat16
    dma = pltpu.SemaphoreType.DMA
    return pl.pallas_call(
        finish_kernel,
        in_specs=[ANY, ANY, ANY, ANY, ANY, VMEM, VMEM, ANY, VMEM, ANY, VMEM],
        out_specs=ANY,
        out_shape=jax.ShapeDtypeStruct((B, S, C), bf16),
        scratch_shapes=[pltpu.VMEM((n, S, C), bf16), pltpu.VMEM((rest, S, C), bf16), pltpu.VMEM((rest, D, C), bf16),
                        pltpu.VMEM((rest, S, C), bf16), pltpu.VMEM((S, D), bf16), pltpu.VMEM((S, 128), jnp.float32),
                        pltpu.VMEM((C, H), bf16), pltpu.VMEM((H, C), bf16),
                        *mlp_scratch(S, C, H), dma((n,)), dma((n,)), dma((rest,)), dma((rest,)), dma((rest,)), dma((4, 2)), dma((2,))],
        compiler_params=pltpu.CompilerParams(vmem_limit_bytes=60 << 20),
        name="finish",
    )(patches, early, g, wt2t, bt2c, s2, o2, w_ch1, b_ch1, w_ch2, b_ch2)


def solution(mesh):
    row_spec = P('dp', 'sp', None)
    side = math.isqrt(mesh.shape['sp'] // 2)

    def local_layer(patches, ln1_scale, ln1_bias, w_tok1, b_tok1, w_tok2, b_tok2, ln2_scale, ln2_bias, w_ch1, b_ch1, w_ch2, b_ch2):
        tail = (ln2_scale, ln2_bias, w_ch1, b_ch1, w_ch2, b_ch2)
        early, g, wt2t, bt2c = exchange(side, patches.shape[0] // 2 - 1, patches, ln1_scale, ln1_bias, w_tok1, b_tok1,
                                        w_tok2, b_tok2[None], *tail)
        return finish(patches, early, g, wt2t, bt2c, *tail)

    return jax.shard_map(local_layer, mesh=mesh, in_specs=(row_spec,) + (P(),) * 12, out_specs=row_spec, check_vma=False)
```
